32 devices in a mesh: section: 4 (over z), seq: 8 (over y, x, core).
Axes of the slice: x: 2, y: 2, z: 4, core: 2. Of those that a mesh axis runs over, the one named last changes fastest.
Arguments:
- saved: bfloat16 [4, 3, 1024, 2304], P('section', None, 'seq'), may hold values from -8 to 8
- cotangent: bfloat16 [3, 1024, 2304], P(None, 'seq'), may hold values from -0.109375 to 0.109375
- slot_table: int32 [4, 3], P('section'), may hold values from 0 to 2, each once within a row
- gain: float32 [4, 2304], P('section'), may hold values from 0.25 to 1.75
- value_weight: bfloat16 [4, 2304, 1024], P('section'), may hold values from -0.125 to 0.125
- out_weight: bfloat16 [4, 2304, 1024], P('section'), may hold values from -0.1875 to 0.1875
Outputs:
- value_grad: float32 [4, 2304, 1024], P('section', 'seq')
- out_grad: float32 [4, 2304, 1024], P('section', 'seq')
- gain_grad: float32 [4, 2304], P('section')
The draws below stay inside these ranges and needn't reach their ends.
Inputs may be any that keep to these rules, and one draw needn't show every extreme that they name: `slot_table`: each row names every stash slot once.
All inputs are finite; a program needn't handle non-finite values.
Results may differ from the reference program's by a relative error of at most 0.007.
Values may be sent and summed in bfloat16 or wider, within the bound.
A program may use at most 128 MiB of HBM per device.

```python
import jax
import jax.numpy as jnp
from jax import lax

D = 2304
R = 1024
MICRO = 3
TOKENS = 1024
N_SECTION = 4


def strengthened(entries, own_key, source, target, shards_of, factor):
    owner, partner = [(jnp.arange(entries.shape[dim]) // (entries.shape[dim] // shards_of)).reshape([-1 if axis == dim else 1 for axis in range(entries.ndim)]) for dim in (source, target)]
    chosen = jax.random.permutation(own_key, shards_of)[partner]
    strong = (owner == chosen) | (owner == (partner + shards_of // 2) % shards_of)
    return jnp.where(strong, factor * entries, entries)


def block_scale(own_key, dims, pieces, low, high):
    loudness = 1.0
    for axis_at, shards_of in pieces:
        steps = jax.random.uniform(jax.random.fold_in(jax.random.fold_in(own_key, 6), axis_at), (shards_of,), jnp.float32, low / len(pieces), high / len(pieces))
        loudness = loudness * jnp.repeat(jnp.exp(steps), dims[axis_at] // shards_of).reshape((-1,) + (1,) * (len(dims) - 1 - axis_at))
    return loudness


def bell_draw(key, extent, spread, limit, shards=(), held_as=jnp.bfloat16):
    entries = spread * jax.random.normal(key, extent, jnp.float32)
    if shards:
        entries = entries * block_scale(key, extent, shards, -0.22, 0.18)
    return jnp.clip(entries, -limit, limit).astype(held_as)


def bell_draw_with(rng, extent, scale, most, shards, heavy, kind=jnp.bfloat16):
    drawn = scale * jax.random.normal(rng, extent, jnp.float32)
    if shards:
        drawn = drawn * block_scale(rng, extent, shards, -0.22, 0.18)
    return jnp.clip(strengthened(drawn, jax.random.fold_in(rng, 3), *heavy), -most, most).astype(kind)


def setup_inputs(seed: int = 0) -> dict:
    splits = jax.random.split(jax.random.key(seed), 7)
    return {
        "saved": bell_draw_with(splits[0], (N_SECTION, MICRO, TOKENS, D), 1.0, 8.0, ((0, 4), (2, 8)), (2, 3, 8, 2.0)),
        "cotangent": bell_draw(splits[1], (MICRO, TOKENS, D), ((MICRO * TOKENS) ** -0.5), 0.109375, ((1, 8),)),
        "slot_table": jax.vmap(lambda own: jax.random.permutation(own, MICRO))(jax.random.split(splits[2], N_SECTION)).reshape((N_SECTION, MICRO)).astype(jnp.int32),
        "gain": jnp.clip(1.0 + 0.15 * jax.random.normal(splits[3], (N_SECTION, D), jnp.float32), 0.25, 1.75),
        "value_weight": bell_draw(splits[4], (N_SECTION, D, R), D ** -0.5, 0.125, ((0, 4),)),
        "out_weight": bell_draw(splits[5], (N_SECTION, D, R), R ** -0.5, 0.1875, ((0, 4),)),
    }


EPSILON = 1e-06

def normalize(inputs, gain_row):
    value_rows = inputs.astype(jnp.float32)
    inv_rms = lax.rsqrt(lax.optimization_barrier(jnp.mean(value_rows * value_rows, axis=-1, keepdims=True)) + EPSILON)
    unit_rows = value_rows * inv_rms
    return (unit_rows, inv_rms, (unit_rows * gain_row).astype(jnp.bfloat16))

def layer_backward(inputs, grad_out, gain_row, w_value, w_out):
    unit_rows, inv_rms, normed = normalize(inputs, gain_row)
    value_out = jnp.dot(normed, w_value, preferred_element_type=jnp.float32).astype(jnp.bfloat16)
    grad_value = jnp.dot(grad_out, w_out, preferred_element_type=jnp.float32).astype(jnp.bfloat16)
    grad_normed = lax.dot_general(grad_value, w_value, (((1,), (1,)), ((), ())), preferred_element_type=jnp.float32)
    gain_term = lax.optimization_barrier(jnp.sum(grad_normed * unit_rows, axis=0))
    grad_unit = grad_normed * gain_row
    grad_in = grad_out.astype(jnp.float32) + inv_rms * (grad_unit - unit_rows * lax.optimization_barrier(jnp.mean(grad_unit * unit_rows, axis=-1, keepdims=True)))
    value_term = lax.dot_general(normed, grad_value, (((0,), (0,)), ((), ())), preferred_element_type=jnp.float32)
    out_term = lax.dot_general(grad_out, value_out, (((0,), (0,)), ((), ())), preferred_element_type=jnp.float32)
    return (grad_in.astype(jnp.bfloat16), gain_term, value_term, out_term)

def reference(saved, cotangent, slot_table, gain, value_weight, out_weight):
    grads = [cotangent[micro_index] for micro_index in range(MICRO)]
    value_list = []
    out_list = []
    gain_list = []
    for section_index in reversed(range(N_SECTION)):
        value_acc = jnp.zeros((D, R), jnp.float32)
        out_acc = jnp.zeros((D, R), jnp.float32)
        gain_acc = jnp.zeros((D,), jnp.float32)
        next_grads = []
        for micro_index in range(MICRO):
            slot_index = slot_table[section_index, micro_index].astype(jnp.int32)
            inputs = lax.dynamic_index_in_dim(saved[section_index], slot_index, 0, keepdims=False)
            grad_in, gain_term, value_term, out_term = layer_backward(inputs, grads[micro_index], gain[section_index], value_weight[section_index], out_weight[section_index])
            value_acc = value_acc + value_term
            out_acc = out_acc + out_term
            gain_acc = gain_acc + gain_term
            next_grads.append(grad_in)
        grads = next_grads
        value_list.insert(0, value_acc)
        out_list.insert(0, out_acc)
        gain_list.insert(0, gain_acc)
    return (jnp.stack(value_list), jnp.stack(out_list), jnp.stack(gain_list))
```

```python
import functools

import jax
import jax.numpy as jnp
from jax import lax
from jax.experimental import pallas as pl
from jax.experimental.pallas import tpu as pltpu
from jax.sharding import PartitionSpec as P

EPSILON = 1e-06


def passed_along(value, axis, steps):
    count = lax.axis_size(axis)
    first, last = (max(0, -steps), min(count, count - steps))
    return lax.ppermute(value, axis, [(source, source + steps) for source in range(first, last)])


def normalize(inputs, gain_row):
    value_rows = inputs.astype(jnp.float32)
    inv_rms = lax.rsqrt(jnp.mean(value_rows * value_rows, axis=-1, keepdims=True) + EPSILON)
    unit_rows = value_rows * inv_rms
    return (unit_rows, inv_rms, (unit_rows * gain_row).astype(jnp.bfloat16))


def input_grads(inputs, grad_out, gain_row, w_value, w_out):
    unit_rows, inv_rms, normed = normalize(inputs, gain_row)
    grad_value = jnp.dot(grad_out, w_out, preferred_element_type=jnp.float32).astype(jnp.bfloat16)
    grad_normed = lax.dot_general(
        grad_value, w_value, (((1,), (1,)), ((), ())), preferred_element_type=jnp.float32
    )
    gain_term = jnp.sum(grad_normed * unit_rows, axis=0)
    grad_unit = grad_normed * gain_row
    grad_in = grad_out.astype(jnp.float32) + inv_rms * (
        grad_unit - unit_rows * jnp.mean(grad_unit * unit_rows, axis=-1, keepdims=True)
    )
    return (grad_in.astype(jnp.bfloat16), grad_value, normed, gain_term)


def arrivals(
    step_index, sent, section_count, section_index, micro_count, cotangent, local_saved, slot_order
):
    if step_index > 0:
        incoming = passed_along(sent, "section", -1)
    else:
        incoming = sent
    micro_index = step_index - (section_count - 1 - section_index)
    active_now = jnp.logical_and(micro_index >= 0, micro_index < micro_count)
    clipped = jnp.clip(micro_index, 0, micro_count - 1)
    top_grad = lax.dynamic_index_in_dim(cotangent, clipped, 0, keepdims=False)
    grad_out = jnp.where(section_index == section_count - 1, top_grad, incoming)
    slot_index = lax.dynamic_index_in_dim(slot_order, clipped, 0, keepdims=False)
    inputs = lax.dynamic_index_in_dim(local_saved, slot_index, 0, keepdims=False)
    return (active_now, clipped, grad_out, inputs)


def per_device(saved, cotangent, slot_table, gain, value_weight, out_weight):
    section_count = lax.axis_size("section")
    section_index = lax.axis_index("section")
    micro_count = slot_table.shape[1]
    local_saved = saved[0]
    slot_order = slot_table[0]
    gain_row = gain[0]
    w_value = value_weight[0]
    w_out = out_weight[0]
    token_rows = cotangent.shape[1]
    model_width = w_value.shape[0]
    inner_width = w_value.shape[1]
    sent = jnp.zeros((token_rows, model_width), jnp.bfloat16)
    gain_acc = jnp.zeros((model_width,), jnp.float32)
    out_stash = jnp.zeros((micro_count, token_rows, model_width), jnp.bfloat16)
    value_stash = jnp.zeros((micro_count, token_rows, inner_width), jnp.bfloat16)
    for step_index in range(micro_count + section_count - 1):
        active_now, clipped, grad_out, inputs = arrivals(
            step_index,
            sent,
            section_count,
            section_index,
            micro_count,
            cotangent,
            local_saved,
            slot_order,
        )

        def working(carried):
            grad_in, grad_value, normed, gain_term = input_grads(
                inputs, grad_out, gain_row, w_value, w_out
            )
            new_out = lax.dynamic_update_index_in_dim(carried[2], grad_out, clipped, 0)
            new_value = lax.dynamic_update_index_in_dim(carried[3], grad_value, clipped, 0)
            return (grad_in, carried[1] + gain_term, new_out, new_value)

        def resting(carried):
            return carried

        sent, gain_acc, out_stash, value_stash = lax.cond(
            active_now, working, resting, (sent, gain_acc, out_stash, value_stash)
        )
    ordered = jnp.take(local_saved, slot_order, axis=0).reshape(
        micro_count * token_rows, model_width
    )
    unit_all, inv_all, normed_all = normalize(ordered, gain_row)
    values_all = jnp.dot(normed_all, w_value, preferred_element_type=jnp.float32).astype(
        jnp.bfloat16
    )
    grads_all = out_stash.reshape(micro_count * token_rows, model_width)
    grad_values = value_stash.reshape(micro_count * token_rows, inner_width)
    value_acc = lax.dot_general(
        normed_all, grad_values, (((0,), (0,)), ((), ())), preferred_element_type=jnp.float32
    )
    out_acc = lax.dot_general(
        grads_all, values_all, (((0,), (0,)), ((), ())), preferred_element_type=jnp.float32
    )
    value_grad, out_grad = (
        lax.psum_scatter(value_acc, "seq", scatter_dimension=0, tiled=True),
        lax.psum_scatter(out_acc, "seq", scatter_dimension=0, tiled=True),
    )
    gain_total = lax.psum(gain_acc, "seq")
    return (value_grad[None], out_grad[None], gain_total[None])


TILE = 256
LANES = 128
CHUNKS = 2
VMEM_BYTES = 60 * 1024 * 1024


def flipped(index, bits, count):
    total, unit = 0, 1
    while unit < count:
        total = total + ((index // unit + (bits // unit) % 2) % 2) * unit
        unit *= 2
    return total


def tile_at(index, size=TILE):
    return pl.ds(pl.multiple_of(index * size, size), size)


def fused_kernel(
    peers,
    sections,
    slot_ref,
    saved_hbm,
    cot_hbm,
    gain_ref,
    wv_hbm,
    wo_hbm,
    vg_ref,
    og_ref,
    gg_ref,
    saved_ref,
    wv_ref,
    wo_ref,
    inv_buf,
    grad_buf,
    pass_buf,
    normed,
    gn,
    rows_all,
    turned,
    cols_all,
    acc,
    part_out,
    part_in,
    gain_all,
    load_sem,
    rows_send,
    rows_recv,
    cols_send,
    cols_recv,
    down_send,
    down_recv,
    part_send,
    part_recv,
    gain_send,
    gain_recv,
):
    section = lax.axis_index("section")
    me = lax.axis_index("seq")
    micro, tokens, width = grad_buf.shape
    inner = wv_ref.shape[1]
    share = width // peers
    wide, narrow = width // TILE, inner // TILE
    chunk = tokens // CHUNKS
    steps = micro * CHUNKS
    top = section == sections - 1
    near = (peers // 4, peers // 2)
    far = (peers // 2, peers // 4)

    def peer(bits):
        return {"seq": flipped(me, bits, peers)}

    def coordinate(device, bit):
        return (device // bit) % 2

    def place(kind, device):
        return coordinate(device, near[kind]) * 2 + device % 2

    def rows_at(kind, m, h, owner):
        if kind == 1:
            return rows_all.at[kind, m, tile_at(place(kind, owner), tokens)]
        return rows_all.at[kind, m, tile_at(place(kind, owner) * CHUNKS + h, chunk)]

    def row_copy(kind, m, h, owner, way, bits):
        spot = rows_at(kind, m, h, owner)
        return pltpu.make_async_remote_copy(
            src_ref=spot,
            dst_ref=spot,
            send_sem=rows_send.at[kind, m, h, way],
            recv_sem=rows_recv.at[kind, m, h, way],
            device_id=peer(bits),
            device_id_type=pl.DeviceIdType.MESH,
        )

    def own_to_core(kind, m, h):
        return row_copy(kind, m, h, me, 0, 1)

    def own_to_chip(kind, m, h):
        return row_copy(kind, m, h, me, 1, near[kind])

    def relay(kind, m, h):
        return row_copy(kind, m, h, flipped(me, near[kind], peers), 2, 1)

    def from_core(kind, m, h):
        return row_copy(kind, m, h, flipped(me, 1, peers), 0, 1)

    def from_chip(kind, m, h):
        return row_copy(kind, m, h, flipped(me, near[kind], peers), 1, near[kind])

    def from_relay(kind, m, h):
        return row_copy(kind, m, h, flipped(me, near[kind] + 1, peers), 2, 1)

    def block_of(kind, device, b):
        return device + (b - coordinate(device, far[kind])) * far[kind]

    def col_copy(kind, m, owner, bits, b):
        target = flipped(me, bits, peers)
        return pltpu.make_async_remote_copy(
            src_ref=turned.at[kind, m, tile_at(block_of(kind, target, b), share)],
            dst_ref=cols_all.at[kind, m, b, :, tile_at(place(kind, owner), tokens)],
            send_sem=cols_send.at[kind, m, bits, b],
            recv_sem=cols_recv.at[kind, m, bits, b],
            device_id=peer(bits),
            device_id_type=pl.DeviceIdType.MESH,
        )

    def ways(kind):
        return (near[kind], near[kind] + 1, 1)

    def down_copy(k, target):
        spot = tile_at(k % CHUNKS, chunk)
        return pltpu.make_async_remote_copy(
            src_ref=pass_buf.at[k // CHUNKS, spot],
            dst_ref=grad_buf.at[k // CHUNKS, spot],
            send_sem=down_send.at[k],
            recv_sem=down_recv.at[k],
            device_id={"section": target},
            device_id_type=pl.DeviceIdType.MESH,
        )

    def part_copy(kind, j):
        return pltpu.make_async_remote_copy(
            src_ref=part_out.at[kind, j],
            dst_ref=part_in.at[kind, j],
            send_sem=part_send.at[kind, j],
            recv_sem=part_recv.at[kind, j],
            device_id=peer(far[kind]),
            device_id_type=pl.DeviceIdType.MESH,
        )

    def gain_copy(owner, bits):
        return pltpu.make_async_remote_copy(
            src_ref=gain_all.at[owner],
            dst_ref=gain_all.at[owner],
            send_sem=gain_send.at[bits],
            recv_sem=gain_recv.at[bits],
            device_id=peer(bits),
            device_id_type=pl.DeviceIdType.MESH,
        )

    load_saved = pltpu.make_async_copy(saved_hbm, saved_ref, load_sem.at[0])
    load_wo = pltpu.make_async_copy(wo_hbm, wo_ref, load_sem.at[1])
    load_wv = pltpu.make_async_copy(wv_hbm, wv_ref, load_sem.at[2])
    load_cot = pltpu.make_async_copy(cot_hbm, grad_buf, load_sem.at[3])
    load_saved.start()

    @pl.when(top)
    def _():
        load_cot.start()

    load_wo.start()
    load_wv.start()

    barrier = pltpu.get_barrier_semaphore()
    for bits in range(1, peers):
        pl.semaphore_signal(
            barrier, inc=1, device_id=peer(bits), device_id_type=pl.DeviceIdType.MESH
        )

    @pl.when(section > 0)
    def _():
        pl.semaphore_signal(
            barrier,
            inc=1,
            device_id={"section": section - 1},
            device_id_type=pl.DeviceIdType.MESH,
        )

    @pl.when(section < sections - 1)
    def _():
        pl.semaphore_signal(
            barrier,
            inc=1,
            device_id={"section": section + 1},
            device_id_type=pl.DeviceIdType.MESH,
        )

    gain_all[me] = jnp.zeros((1, width), jnp.float32)
    load_saved.wait()

    def scales(m, carry):
        slot = slot_ref[0, m]

        def squares(j, total):
            x = saved_ref[slot, :, tile_at(j)].astype(jnp.float32)
            return total + jnp.sum(x * x, axis=1, keepdims=True)

        total = lax.fori_loop(0, wide, squares, jnp.zeros((tokens, 1), jnp.float32))
        inv_buf[m] = lax.rsqrt(total / width + EPSILON)
        return carry

    lax.fori_loop(0, micro, scales, 0)

    @pl.when(top)
    def _():
        load_cot.wait()

    load_wo.wait()
    load_wv.wait()
    pl.semaphore_wait(
        barrier,
        peers - 1
        + (section > 0).astype(jnp.int32)
        + (section < sections - 1).astype(jnp.int32),
    )

    def send_cols(kind, m):
        for bits in ways(kind):
            for b in range(2):
                col_copy(kind, m, me, bits, b).start()
        for b in range(2):
            cols_all[kind, m, b, :, tile_at(place(kind, me), tokens)] = turned[
                kind, m, tile_at(block_of(kind, me, b), share)
            ]

    def values(m):
        slot = slot_ref[0, m]
        inv = inv_buf[m]

        def norm(j, carry):
            x = saved_ref[slot, :, tile_at(j)].astype(jnp.float32)
            n = (x * inv * gain_ref[:, tile_at(j)]).astype(jnp.bfloat16)
            normed[:, tile_at(j)] = n
            turned[0, m, tile_at(j)] = n.T
            return carry

        lax.fori_loop(0, wide, norm, 0)
        send_cols(0, m)

        def project(j, carry):
            rows_all[1, m, tile_at(place(1, me), tokens), tile_at(j)] = jnp.dot(
                normed[...], wv_ref[:, tile_at(j)], preferred_element_type=jnp.float32
            ).astype(jnp.bfloat16)
            return carry

        lax.fori_loop(0, narrow, project, 0)
        own_to_chip(1, m, 0).start()
        own_to_core(1, m, 0).start()

    def turn(m):
        def tile(j, carry):
            turned[1, m, tile_at(j)] = grad_buf[m, :, tile_at(j)].T
            return carry

        lax.fori_loop(0, wide, tile, 0)
        send_cols(1, m)

    def chain(k):
        m, h = k // CHUNKS, k % CHUNKS
        here = tile_at(h, chunk)
        slot = slot_ref[0, m]
        inv = inv_buf[m, here]
        mine = tile_at(place(0, me) * CHUNKS + h, chunk)

        @pl.when(section < sections - 1)
        def _():
            down_copy(k, section + 1).wait_recv()

        def project(j, carry):
            rows_all[0, m, mine, tile_at(j)] = jnp.dot(
                grad_buf[m, here], wo_ref[:, tile_at(j)], preferred_element_type=jnp.float32
            ).astype(jnp.bfloat16)
            return carry

        lax.fori_loop(0, narrow, project, 0)
        own_to_chip(0, m, h).start()
        own_to_core(0, m, h).start()

        @pl.when(jnp.logical_and(section == 0, h == CHUNKS - 1))
        def _():
            turn(m)

        def back(j, total):
            term = lax.dot_general(
                rows_all[0, m, mine],
                wv_ref[tile_at(j)],
                (((1,), (1,)), ((), ())),
                preferred_element_type=jnp.float32,
            )
            unit = saved_ref[slot, here, tile_at(j)].astype(jnp.float32) * inv
            gn[:, tile_at(j)] = term
            both = term * unit
            gain_all[me, :, tile_at(j)] += jnp.sum(both, axis=0, keepdims=True)
            return total + jnp.sum(both * gain_ref[:, tile_at(j)], axis=1, keepdims=True)

        total = lax.fori_loop(0, wide, back, jnp.zeros((chunk, 1), jnp.float32))
        mean = total / width

        @pl.when(section > 0)
        def _():
            def step(j, carry):
                unit = saved_ref[slot, here, tile_at(j)].astype(jnp.float32) * inv
                grad_unit = gn[:, tile_at(j)] * gain_ref[:, tile_at(j)]
                pass_buf[m, here, tile_at(j)] = (
                    grad_buf[m, here, tile_at(j)].astype(jnp.float32)
                    + inv * (grad_unit - unit * mean)
                ).astype(jnp.bfloat16)
                return carry

            lax.fori_loop(0, wide, step, 0)
            down_copy(k, section - 1).start()

        @pl.when(jnp.logical_and(section > 0, h == CHUNKS - 1))
        def _():
            turn(m)

    def relay_values():
        def one(m, carry):
            from_chip(1, m, 0).wait_recv()
            relay(1, m, 0).start()
            return carry

        lax.fori_loop(0, micro, one, 0)

    def relay_grads(k):
        from_chip(0, k // CHUNKS, k % CHUNKS).wait_recv()
        relay(0, k // CHUNKS, k % CHUNKS).start()

    def gather(kind, m):
        for bits in ways(kind):
            for b in range(2):
                col_copy(kind, m, flipped(me, bits, peers), bits, b).wait_recv()
        for h in range(CHUNKS if kind == 0 else 1):
            from_core(kind, m, h).wait_recv()
            from_relay(kind, m, h).wait_recv()

    def product(kind, m, b, j):
        return jnp.dot(
            cols_all[kind, m, b],
            rows_all[kind, m, :, tile_at(j)],
            preferred_element_type=jnp.float32,
        )

    def weights(m):
        for kind in (0, 1):
            gather(kind, m)

            def tile(i, carry):
                b, j = i // narrow, i % narrow
                acc[kind, b, :, tile_at(j)] += product(kind, m, b, j)
                return carry

            lax.fori_loop(0, 2 * narrow, tile, 0)

    @pl.when(section > 0)
    def _():
        acc[...] = jnp.zeros_like(acc)

    def stage(t, carry):
        at_top = top.astype(jnp.int32)
        paired = (t < 2 * micro).astype(jnp.int32)
        chained = at_top * (1 - paired * (t % 2)) + (1 - at_top) * (t >= micro).astype(jnp.int32)
        k = at_top * (paired * (t // 2) + (1 - paired) * (t - micro)) + (1 - at_top) * (t - micro)
        m = at_top * (t // 2) + (1 - at_top) * t

        @pl.when(chained == 1)
        def _():
            @pl.when(jnp.logical_and(section == 0, k == 0))
            def _():
                acc[...] = jnp.zeros_like(acc)
                relay_values()

            chain(k)

            @pl.when(jnp.logical_and(section == 0, k > 0))
            def _():
                relay_grads(k - 1)

            @pl.when(
                jnp.logical_and(
                    section == 0, jnp.logical_and(k > CHUNKS, (k - 1) % CHUNKS == 0)
                )
            )
            def _():
                weights((k - 1) // CHUNKS - 1)

        @pl.when(chained == 0)
        def _():
            values(m)

        return carry

    lax.fori_loop(0, steps + micro, stage, 0)
    for bits in range(1, peers):
        gain_copy(me, bits).start()

    @pl.when(section > 0)
    def _():
        relay_values()

        def early(k, carry):
            relay_grads(k)
            return carry

        lax.fori_loop(0, steps - 1, early, 0)

        def heavy(m, carry):
            weights(m)
            return carry

        lax.fori_loop(0, micro - 1, heavy, 0)

    relay_grads(steps - 1)
    last = micro - 1
    for kind in (0, 1):
        gather(kind, last)
        mine = coordinate(me, far[kind])

        def given(j, carry):
            part_out[kind, j] = (
                acc[kind, 1 - mine, :, tile_at(j)] + product(kind, last, 1 - mine, j)
            ).astype(jnp.bfloat16)
            part_copy(kind, j).start()
            return carry

        lax.fori_loop(0, narrow, given, 0)

    for kind in (0, 1):
        mine = coordinate(me, far[kind])

        def kept(j, carry):
            acc[kind, mine, :, tile_at(j)] += product(kind, last, mine, j)
            return carry

        lax.fori_loop(0, narrow, kept, 0)

    for bits in range(1, peers):
        gain_copy(flipped(me, bits, peers), bits).wait_recv()
    gained = gain_all[0]
    for owner in range(1, peers):
        gained = gained + gain_all[owner]
    gg_ref[...] = gained

    for kind, out_ref in ((0, vg_ref), (1, og_ref)):
        mine = coordinate(me, far[kind])

        def join(j, carry):
            part_copy(kind, j).wait_recv()
            out_ref[:, tile_at(j)] = acc[kind, mine, :, tile_at(j)] + part_in[kind, j].astype(
                jnp.float32
            )
            return carry

        lax.fori_loop(0, narrow, join, 0)

    def drain(m, carry):
        for kind in (0, 1):
            for bits in ways(kind):
                for b in range(2):
                    col_copy(kind, m, me, bits, b).wait_send()
            for h in range(CHUNKS if kind == 0 else 1):
                own_to_core(kind, m, h).wait_send()
                own_to_chip(kind, m, h).wait_send()
                relay(kind, m, h).wait_send()
        return carry

    lax.fori_loop(0, micro, drain, 0)

    @pl.when(section > 0)
    def _():
        def sent(k, carry):
            down_copy(k, section - 1).wait_send()
            return carry

        lax.fori_loop(0, steps, sent, 0)

    for kind in (0, 1):
        for j in range(narrow):
            part_copy(kind, j).wait_send()
    for bits in range(1, peers):
        gain_copy(me, bits).wait_send()


def fused(mesh, saved, cotangent, slot_table, gain, value_weight, out_weight):
    peers, sections = mesh.shape["seq"], mesh.shape["section"]
    micro, tokens, width = cotangent.shape
    inner = value_weight.shape[2]
    share = width // peers
    narrow = inner // TILE
    chunk = tokens // CHUNKS
    held = pl.BlockSpec(memory_space=pltpu.VMEM)
    far_off = pl.BlockSpec(memory_space=pl.ANY)
    value_grad, out_grad, gain_grad = pl.pallas_call(
        functools.partial(fused_kernel, peers, sections),
        out_shape=(
            jax.ShapeDtypeStruct((share, inner), jnp.float32),
            jax.ShapeDtypeStruct((share, inner), jnp.float32),
            jax.ShapeDtypeStruct((1, width), jnp.float32),
        ),
        in_specs=[
            pl.BlockSpec(memory_space=pltpu.SMEM),
            far_off,
            far_off,
            held,
            far_off,
            far_off,
        ],
        out_specs=(held, held, held),
        scratch_shapes=[
            pltpu.VMEM((micro, tokens, width), jnp.bfloat16),
            pltpu.VMEM((width, inner), jnp.bfloat16),
            pltpu.VMEM((width, inner), jnp.bfloat16),
            pltpu.VMEM((micro, tokens, 1), jnp.float32),
            pltpu.VMEM((micro, tokens, width), jnp.bfloat16),
            pltpu.VMEM((micro, tokens, width), jnp.bfloat16),
            pltpu.VMEM((tokens, width), jnp.bfloat16),
            pltpu.VMEM((chunk, width), jnp.float32),
            pltpu.VMEM((2, micro, 4 * tokens, inner), jnp.bfloat16),
            pltpu.VMEM((2, micro, width, tokens), jnp.bfloat16),
            pltpu.VMEM((2, micro, 2, share, 4 * tokens), jnp.bfloat16),
            pltpu.VMEM((2, 2, share, inner), jnp.float32),
            pltpu.VMEM((2, narrow, share, TILE), jnp.bfloat16),
            pltpu.VMEM((2, narrow, share, TILE), jnp.bfloat16),
            pltpu.VMEM((peers, 1, width), jnp.float32),
            pltpu.SemaphoreType.DMA((4,)),
            pltpu.SemaphoreType.DMA((2, micro, CHUNKS, 3)),
            pltpu.SemaphoreType.DMA((2, micro, CHUNKS, 3)),
            pltpu.SemaphoreType.DMA((2, micro, peers, 2)),
            pltpu.SemaphoreType.DMA((2, micro, peers, 2)),
            pltpu.SemaphoreType.DMA((micro * CHUNKS,)),
            pltpu.SemaphoreType.DMA((micro * CHUNKS,)),
            pltpu.SemaphoreType.DMA((2, narrow)),
            pltpu.SemaphoreType.DMA((2, narrow)),
            pltpu.SemaphoreType.DMA((peers,)),
            pltpu.SemaphoreType.DMA((peers,)),
        ],
        compiler_params=pltpu.CompilerParams(
            collective_id=0, has_side_effects=True, vmem_limit_bytes=VMEM_BYTES
        ),
    )(slot_table, saved[0], cotangent, gain, value_weight[0], out_weight[0])
    return value_grad[None], out_grad[None], gain_grad


def fits(mesh, saved, cotangent, slot_table, gain, value_weight, out_weight):
    peers = mesh.shape["seq"]
    micro, tokens, width = cotangent.shape
    inner = value_weight.shape[2]
    share = width // peers
    held = 4 * width * inner + 2 * 2 * micro * 4 * tokens * (inner + 2 * share)
    held += 2 * micro * tokens * width * 5 + 6 * tokens * width
    held += share * inner * (4 * 4 + 4 * 2 + 4 * 2)
    return (
        peers == 8
        and tokens % LANES == 0
        and width % TILE == 0
        and inner % TILE == 0
        and width % (16 * peers) == 0
        and held < VMEM_BYTES - 4 * 1024 * 1024
    )


def on_device(mesh, *arrays):
    if fits(mesh, *arrays):
        return fused(mesh, *arrays)
    return per_device(*arrays)


def solution(mesh):
    in_specs = (
        P("section", None, "seq", None),
        P(None, "seq", None),
        P("section", None),
        P("section", None),
        P("section", None, None),
        P("section", None, None),
    )
    out_specs = (P("section", "seq", None), P("section", "seq", None), P("section", None))
    return jax.shard_map(
        functools.partial(on_device, mesh), mesh=mesh, in_specs=in_specs, out_specs=out_specs, check_vma=False
    )
```

```python
import functools

import jax
import jax.numpy as jnp
from jax import lax
from jax.experimental import pallas as pl
from jax.experimental.pallas import tpu as pltpu
from jax.sharding import PartitionSpec as P

EPSILON = 1e-06


def passed_along(value, axis, steps):
    count = lax.axis_size(axis)
    first, last = (max(0, -steps), min(count, count - steps))
    return lax.ppermute(value, axis, [(source, source + steps) for source in range(first, last)])


def normalize(inputs, gain_row):
    value_rows = inputs.astype(jnp.float32)
    inv_rms = lax.rsqrt(jnp.mean(value_rows * value_rows, axis=-1, keepdims=True) + EPSILON)
    unit_rows = value_rows * inv_rms
    return (unit_rows, inv_rms, (unit_rows * gain_row).astype(jnp.bfloat16))


def input_grads(inputs, grad_out, gain_row, w_value, w_out):
    unit_rows, inv_rms, normed = normalize(inputs, gain_row)
    grad_value = jnp.dot(grad_out, w_out, preferred_element_type=jnp.float32).astype(jnp.bfloat16)
    grad_normed = lax.dot_general(
        grad_value, w_value, (((1,), (1,)), ((), ())), preferred_element_type=jnp.float32
    )
    gain_term = jnp.sum(grad_normed * unit_rows, axis=0)
    grad_unit = grad_normed * gain_row
    grad_in = grad_out.astype(jnp.float32) + inv_rms * (
        grad_unit - unit_rows * jnp.mean(grad_unit * unit_rows, axis=-1, keepdims=True)
    )
    return (grad_in.astype(jnp.bfloat16), grad_value, normed, gain_term)


def arrivals(
    step_index, sent, section_count, section_index, micro_count, cotangent, local_saved, slot_order
):
    if step_index > 0:
        incoming = passed_along(sent, "section", -1)
    else:
        incoming = sent
    micro_index = step_index - (section_count - 1 - section_index)
    active_now = jnp.logical_and(micro_index >= 0, micro_index < micro_count)
    clipped = jnp.clip(micro_index, 0, micro_count - 1)
    top_grad = lax.dynamic_index_in_dim(cotangent, clipped, 0, keepdims=False)
    grad_out = jnp.where(section_index == section_count - 1, top_grad, incoming)
    slot_index = lax.dynamic_index_in_dim(slot_order, clipped, 0, keepdims=False)
    inputs = lax.dynamic_index_in_dim(local_saved, slot_index, 0, keepdims=False)
    return (active_now, clipped, grad_out, inputs)


def per_device(saved, cotangent, slot_table, gain, value_weight, out_weight):
    section_count = lax.axis_size("section")
    section_index = lax.axis_index("section")
    micro_count = slot_table.shape[1]
    local_saved = saved[0]
    slot_order = slot_table[0]
    gain_row = gain[0]
    w_value = value_weight[0]
    w_out = out_weight[0]
    token_rows = cotangent.shape[1]
    model_width = w_value.shape[0]
    inner_width = w_value.shape[1]
    sent = jnp.zeros((token_rows, model_width), jnp.bfloat16)
    gain_acc = jnp.zeros((model_width,), jnp.float32)
    out_stash = jnp.zeros((micro_count, token_rows, model_width), jnp.bfloat16)
    value_stash = jnp.zeros((micro_count, token_rows, inner_width), jnp.bfloat16)
    for step_index in range(micro_count + section_count - 1):
        active_now, clipped, grad_out, inputs = arrivals(
            step_index,
            sent,
            section_count,
            section_index,
            micro_count,
            cotangent,
            local_saved,
            slot_order,
        )

        def working(carried):
            grad_in, grad_value, normed, gain_term = input_grads(
                inputs, grad_out, gain_row, w_value, w_out
            )
            new_out = lax.dynamic_update_index_in_dim(carried[2], grad_out, clipped, 0)
            new_value = lax.dynamic_update_index_in_dim(carried[3], grad_value, clipped, 0)
            return (grad_in, carried[1] + gain_term, new_out, new_value)

        def resting(carried):
            return carried

        sent, gain_acc, out_stash, value_stash = lax.cond(
            active_now, working, resting, (sent, gain_acc, out_stash, value_stash)
        )
    ordered = jnp.take(local_saved, slot_order, axis=0).reshape(
        micro_count * token_rows, model_width
    )
    unit_all, inv_all, normed_all = normalize(ordered, gain_row)
    values_all = jnp.dot(normed_all, w_value, preferred_element_type=jnp.float32).astype(
        jnp.bfloat16
    )
    grads_all = out_stash.reshape(micro_count * token_rows, model_width)
    grad_values = value_stash.reshape(micro_count * token_rows, inner_width)
    value_acc = lax.dot_general(
        normed_all, grad_values, (((0,), (0,)), ((), ())), preferred_element_type=jnp.float32
    )
    out_acc = lax.dot_general(
        grads_all, values_all, (((0,), (0,)), ((), ())), preferred_element_type=jnp.float32
    )
    value_grad, out_grad = (
        lax.psum_scatter(value_acc, "seq", scatter_dimension=0, tiled=True),
        lax.psum_scatter(out_acc, "seq", scatter_dimension=0, tiled=True),
    )
    gain_total = lax.psum(gain_acc, "seq")
    return (value_grad[None], out_grad[None], gain_total[None])


TILE = 256
LANES = 128
CHUNKS = 2
VMEM_BYTES = 60 * 1024 * 1024


def flipped(index, bits, count):
    total, unit = 0, 1
    while unit < count:
        total = total + ((index // unit + (bits // unit) % 2) % 2) * unit
        unit *= 2
    return total


def tile_at(index, size=TILE):
    return pl.ds(pl.multiple_of(index * size, size), size)


def fused_kernel(
    peers,
    sections,
    slot_ref,
    saved_hbm,
    cot_hbm,
    gain_ref,
    wv_hbm,
    wo_hbm,
    vg_ref,
    og_ref,
    gg_ref,
    saved_ref,
    wv_ref,
    wo_ref,
    wvt_ref,
    inv_buf,
    grad_buf,
    pass_buf,
    normed,
    gn,
    rows_all,
    turned,
    cols_all,
    acc,
    part_out,
    part_in,
    gain_part,
    gain_all,
    load_sem,
    out_sem,
    rows_send,
    rows_recv,
    cols_send,
    cols_recv,
    down_send,
    down_recv,
    part_send,
    part_recv,
    gain_send,
    gain_recv,
):
    section = lax.axis_index("section")
    me = lax.axis_index("seq")
    micro, tokens, width = grad_buf.shape
    inner = wv_ref.shape[1]
    share = width // peers
    wide, narrow = width // TILE, inner // TILE
    chunk = tokens // CHUNKS
    steps = micro * CHUNKS
    top = section == sections - 1
    near = (peers // 4, peers // 2)
    far = (peers // 2, peers // 4)

    def peer(bits):
        return {"seq": flipped(me, bits, peers)}

    def coordinate(device, bit):
        return (device // bit) % 2

    def place(kind, device):
        return coordinate(device, near[kind]) * 2 + device % 2

    def rows_at(kind, m, h, owner):
        if kind == 1:
            return rows_all.at[kind, m, tile_at(place(kind, owner), tokens)]
        return rows_all.at[kind, m, tile_at(place(kind, owner) * CHUNKS + h, chunk)]

    def row_copy(kind, m, h, owner, way, bits):
        spot = rows_at(kind, m, h, owner)
        return pltpu.make_async_remote_copy(
            src_ref=spot,
            dst_ref=spot,
            send_sem=rows_send.at[kind, m, h, way],
            recv_sem=rows_recv.at[kind, m, h, way],
            device_id=peer(bits),
            device_id_type=pl.DeviceIdType.MESH,
        )

    def own_to_core(kind, m, h):
        return row_copy(kind, m, h, me, 0, 1)

    def own_to_chip(kind, m, h):
        return row_copy(kind, m, h, me, 1, near[kind])

    def relay(kind, m, h):
        return row_copy(kind, m, h, flipped(me, near[kind], peers), 2, 1)

    def from_core(kind, m, h):
        return row_copy(kind, m, h, flipped(me, 1, peers), 0, 1)

    def from_chip(kind, m, h):
        return row_copy(kind, m, h, flipped(me, near[kind], peers), 1, near[kind])

    def from_relay(kind, m, h):
        return row_copy(kind, m, h, flipped(me, near[kind] + 1, peers), 2, 1)

    def block_of(kind, device, b):
        return device + (b - coordinate(device, far[kind])) * far[kind]

    def col_copy(kind, m, owner, bits, b):
        target = flipped(me, bits, peers)
        return pltpu.make_async_remote_copy(
            src_ref=turned.at[kind, m, tile_at(block_of(kind, target, b), share)],
            dst_ref=cols_all.at[kind, m, b, :, tile_at(place(kind, owner), tokens)],
            send_sem=cols_send.at[kind, m, bits, b],
            recv_sem=cols_recv.at[kind, m, bits, b],
            device_id=peer(bits),
            device_id_type=pl.DeviceIdType.MESH,
        )

    def ways(kind):
        return (near[kind], near[kind] + 1, 1)

    def down_copy(k, target):
        spot = tile_at(k % CHUNKS, chunk)
        return pltpu.make_async_remote_copy(
            src_ref=pass_buf.at[k // CHUNKS, spot],
            dst_ref=grad_buf.at[k // CHUNKS, spot],
            send_sem=down_send.at[k],
            recv_sem=down_recv.at[k],
            device_id={"section": target},
            device_id_type=pl.DeviceIdType.MESH,
        )

    def part_copy(kind, j):
        return pltpu.make_async_remote_copy(
            src_ref=part_out.at[kind, j],
            dst_ref=part_in.at[kind, j],
            send_sem=part_send.at[kind, j],
            recv_sem=part_recv.at[kind, j],
            device_id=peer(far[kind]),
            device_id_type=pl.DeviceIdType.MESH,
        )

    def gain_copy(owner, bits):
        return pltpu.make_async_remote_copy(
            src_ref=gain_all.at[owner],
            dst_ref=gain_all.at[owner],
            send_sem=gain_send.at[bits],
            recv_sem=gain_recv.at[bits],
            device_id=peer(bits),
            device_id_type=pl.DeviceIdType.MESH,
        )

    load_saved = pltpu.make_async_copy(saved_hbm, saved_ref, load_sem.at[0])
    load_wo = pltpu.make_async_copy(wo_hbm, wo_ref, load_sem.at[1])
    load_wv = pltpu.make_async_copy(wv_hbm, wv_ref, load_sem.at[2])
    load_cot = pltpu.make_async_copy(cot_hbm, grad_buf, load_sem.at[3])
    load_saved.start()

    @pl.when(top)
    def _():
        load_cot.start()
        load_wo.start()
        load_wv.start()

    @pl.when(section < sections - 1)
    def _():
        load_wv.start()
        load_wo.start()

    barrier = pltpu.get_barrier_semaphore()
    for bits in range(1, peers):
        pl.semaphore_signal(
            barrier, inc=1, device_id=peer(bits), device_id_type=pl.DeviceIdType.MESH
        )

    @pl.when(section > 0)
    def _():
        pl.semaphore_signal(
            barrier,
            inc=1,
            device_id={"section": section - 1},
            device_id_type=pl.DeviceIdType.MESH,
        )

    @pl.when(section < sections - 1)
    def _():
        pl.semaphore_signal(
            barrier,
            inc=1,
            device_id={"section": section + 1},
            device_id_type=pl.DeviceIdType.MESH,
        )

    gain_part[...] = jnp.zeros_like(gain_part)
    load_saved.wait()

    def scales(m, carry):
        slot = slot_ref[0, m]

        total = jnp.zeros((tokens, LANES), jnp.float32)
        for j in range(width // LANES):
            x = saved_ref[slot, :, j * LANES : (j + 1) * LANES].astype(jnp.float32)
            total = total + x * x
        total = jnp.sum(total, axis=1, keepdims=True)
        inv_buf[m] = lax.rsqrt(total / width + EPSILON)
        return carry

    lax.fori_loop(0, micro, scales, 0)

    @pl.when(top)
    def _():
        load_cot.wait()

    @pl.when(section < sections - 1)
    def _():
        load_wv.wait()

    load_wo.wait()
    pl.semaphore_wait(
        barrier,
        peers - 1
        + (section > 0).astype(jnp.int32)
        + (section < sections - 1).astype(jnp.int32),
    )

    def send_cols(kind, m):
        for bits in ways(kind):
            for b in range(2):
                col_copy(kind, m, me, bits, b).start()
        for b in range(2):
            cols_all[kind, m, b, :, tile_at(place(kind, me), tokens)] = turned[
                kind, m, tile_at(block_of(kind, me, b), share)
            ]

    def values(m):
        slot = slot_ref[0, m]
        inv = inv_buf[m]

        for j in range(wide):
            cols = slice(j * TILE, (j + 1) * TILE)
            x = saved_ref[slot, :, cols].astype(jnp.float32)
            n = (x * inv * gain_ref[:, cols]).astype(jnp.bfloat16)
            normed[:, cols] = n
            turned[0, m, cols] = n.T
        send_cols(0, m)
        rows_all[1, m, tile_at(place(1, me), tokens)] = jnp.dot(
            normed[...], wv_ref[...], preferred_element_type=jnp.float32
        ).astype(jnp.bfloat16)
        own_to_chip(1, m, 0).start()
        own_to_core(1, m, 0).start()

    def turn(m):
        for j in range(wide):
            cols = slice(j * TILE, (j + 1) * TILE)
            turned[1, m, cols] = grad_buf[m, :, cols].T
        send_cols(1, m)

    def chain(k):
        m, h = k // CHUNKS, k % CHUNKS
        here = tile_at(h, chunk)
        slot = slot_ref[0, m]
        inv = inv_buf[m, here]
        mine = tile_at(place(0, me) * CHUNKS + h, chunk)

        @pl.when(section < sections - 1)
        def _():
            down_copy(k, section + 1).wait_recv()

        @pl.when(jnp.logical_and(section == 0, h == CHUNKS - 1))
        def _():
            turn(m)

        rows_all[0, m, mine] = jnp.dot(
            grad_buf[m, here], wo_ref[...], preferred_element_type=jnp.float32
        ).astype(jnp.bfloat16)
        own_to_chip(0, m, h).start()
        own_to_core(0, m, h).start()

        def back(flip):
            grad_value = rows_all[0, m, mine]
            total = jnp.zeros((chunk, LANES), jnp.float32)
            for j in range(wide // 3):
                cols = slice(j * 3 * TILE, (j + 1) * 3 * TILE)
                if flip:
                    term = lax.dot_general(
                        grad_value,
                        wv_ref[cols],
                        (((1,), (1,)), ((), ())),
                        preferred_element_type=jnp.float32,
                    )
                else:
                    term = jnp.dot(
                        grad_value, wvt_ref[:, cols], preferred_element_type=jnp.float32
                    )
                unit = saved_ref[slot, here, cols].astype(jnp.float32) * inv
                grad_unit = term * gain_ref[:, cols]
                gn[:, cols] = grad_unit
                gain_part[:, cols] += jnp.sum(
                    (term * unit).reshape(chunk // 8, 8, 3 * TILE), axis=0
                )
                both = grad_unit * unit
                for i in range(3 * TILE // LANES):
                    total = total + both[:, i * LANES : (i + 1) * LANES]
            return jnp.sum(total, axis=1, keepdims=True) / width

        def down(mean):
            pull = inv * inv * mean
            for j in range(wide):
                cols = slice(j * TILE, (j + 1) * TILE)
                pass_buf[m, here, cols] = (
                    grad_buf[m, here, cols].astype(jnp.float32)
                    + inv * gn[:, cols]
                    - saved_ref[slot, here, cols].astype(jnp.float32) * pull
                ).astype(jnp.bfloat16)
            down_copy(k, section - 1).start()

        @pl.when(top)
        def _():
            @pl.when(k == 0)
            def _():
                load_wv.wait()

            down(back(True))

        @pl.when(section < sections - 1)
        def _():
            mean = back(False)

            @pl.when(section > 0)
            def _():
                down(mean)

        @pl.when(jnp.logical_and(section > 0, h == CHUNKS - 1))
        def _():
            turn(m)

    def relay_values():
        def one(m, carry):
            from_chip(1, m, 0).wait_recv()
            relay(1, m, 0).start()
            return carry

        lax.fori_loop(0, micro, one, 0)

    def relay_grads(k):
        from_chip(0, k // CHUNKS, k % CHUNKS).wait_recv()
        relay(0, k // CHUNKS, k % CHUNKS).start()

    def gather(kind, m):
        for bits in ways(kind):
            for b in range(2):
                col_copy(kind, m, flipped(me, bits, peers), bits, b).wait_recv()
        for h in range(CHUNKS if kind == 0 else 1):
            from_core(kind, m, h).wait_recv()
            from_relay(kind, m, h).wait_recv()

    def product(kind, m, b, cols):
        return jnp.dot(
            cols_all[kind, m, b],
            rows_all[kind, m, :, cols],
            preferred_element_type=jnp.float32,
        )

    def weights(m):
        for kind in (0, 1):
            gather(kind, m)
            both = cols_all[kind, m].reshape(2 * share, 4 * tokens)
            for j in range(inner // (2 * TILE)):
                cols = slice(j * 2 * TILE, (j + 1) * 2 * TILE)
                acc[kind, :, :, cols] += jnp.dot(
                    both, rows_all[kind, m, :, cols], preferred_element_type=jnp.float32
                ).reshape(2, share, 2 * TILE)

    def transpose_weights():
        def tile(j, carry):
            wvt_ref[:, tile_at(j)] = wv_ref[tile_at(j)].T
            return carry

        lax.fori_loop(0, wide, tile, 0)

    def stage(t, carry):
        at_top = top.astype(jnp.int32)
        paired = (t < 2 * micro).astype(jnp.int32)
        chained = at_top * (1 - paired * (t % 2)) + (1 - at_top) * (t >= micro).astype(jnp.int32)
        k = at_top * (paired * (t // 2) + (1 - paired) * (t - micro)) + (1 - at_top) * (t - micro)
        m = at_top * (t // 2) + (1 - at_top) * t

        @pl.when(chained == 1)
        def _():
            @pl.when(jnp.logical_and(section < sections - 1, k == 0))
            def _():
                transpose_weights()

            @pl.when(jnp.logical_and(section == 0, k == 0))
            def _():
                acc[...] = jnp.zeros_like(acc)
                relay_values()

            chain(k)

            @pl.when(jnp.logical_and(section == 0, k > 0))
            def _():
                relay_grads(k - 1)

            @pl.when(
                jnp.logical_and(
                    section == 0, jnp.logical_and(k > CHUNKS, (k - 1) % CHUNKS == 0)
                )
            )
            def _():
                weights((k - 1) // CHUNKS - 1)

        @pl.when(chained == 0)
        def _():
            values(m)

        return carry

    lax.fori_loop(0, steps + micro, stage, 0)
    gain_all[me] = jnp.sum(gain_part[...], axis=0, keepdims=True)
    for bits in range(1, peers):
        gain_copy(me, bits).start()

    @pl.when(section > 0)
    def _():
        acc[...] = jnp.zeros_like(acc)
        relay_values()

        def early(k, carry):
            relay_grads(k)
            return carry

        lax.fori_loop(0, steps - 1, early, 0)

        def heavy(m, carry):
            weights(m)
            return carry

        lax.fori_loop(0, micro - 1, heavy, 0)

    relay_grads(steps - 1)
    last = micro - 1
    for kind in (0, 1):
        gather(kind, last)
        mine = coordinate(me, far[kind])

        for j in range(narrow):
            cols = slice(j * TILE, (j + 1) * TILE)
            part_out[kind, j] = (
                acc[kind, 1 - mine, :, cols] + product(kind, last, 1 - mine, cols)
            ).astype(jnp.bfloat16)
            part_copy(kind, j).start()

    for kind in (0, 1):
        mine = coordinate(me, far[kind])
        for j in range(narrow):
            cols = slice(j * TILE, (j + 1) * TILE)
            acc[kind, mine, :, cols] += product(kind, last, mine, cols)

    for bits in range(1, peers):
        gain_copy(flipped(me, bits, peers), bits).wait_recv()
    gained = gain_all[0]
    for owner in range(1, peers):
        gained = gained + gain_all[owner]
    gg_ref[...] = gained

    def out_copy(kind, j):
        return pltpu.make_async_copy(
            acc.at[kind, coordinate(me, far[kind]), :, tile_at(j)],
            (vg_ref, og_ref)[kind].at[:, tile_at(j)],
            out_sem.at[kind, j],
        )

    for kind in (0, 1):
        mine = coordinate(me, far[kind])
        for j in range(narrow):
            cols = slice(j * TILE, (j + 1) * TILE)
            part_copy(kind, j).wait_recv()
            acc[kind, mine, :, cols] += part_in[kind, j].astype(jnp.float32)
            out_copy(kind, j).start()

    def drain(m, carry):
        for kind in (0, 1):
            for bits in ways(kind):
                for b in range(2):
                    col_copy(kind, m, me, bits, b).wait_send()
            for h in range(CHUNKS if kind == 0 else 1):
                own_to_core(kind, m, h).wait_send()
                own_to_chip(kind, m, h).wait_send()
                relay(kind, m, h).wait_send()
        return carry

    lax.fori_loop(0, micro, drain, 0)

    @pl.when(section > 0)
    def _():
        def sent(k, carry):
            down_copy(k, section - 1).wait_send()
            return carry

        lax.fori_loop(0, steps, sent, 0)

    for kind in (0, 1):
        for j in range(narrow):
            part_copy(kind, j).wait_send()
            out_copy(kind, j).wait()
    for bits in range(1, peers):
        gain_copy(me, bits).wait_send()


def fused(mesh, saved, cotangent, slot_table, gain, value_weight, out_weight):
    peers, sections = mesh.shape["seq"], mesh.shape["section"]
    micro, tokens, width = cotangent.shape
    inner = value_weight.shape[2]
    share = width // peers
    narrow = inner // TILE
    chunk = tokens // CHUNKS
    held = pl.BlockSpec(memory_space=pltpu.VMEM)
    far_off = pl.BlockSpec(memory_space=pl.ANY)
    value_grad, out_grad, gain_grad = pl.pallas_call(
        functools.partial(fused_kernel, peers, sections),
        out_shape=(
            jax.ShapeDtypeStruct((share, inner), jnp.float32),
            jax.ShapeDtypeStruct((share, inner), jnp.float32),
            jax.ShapeDtypeStruct((1, width), jnp.float32),
        ),
        in_specs=[
            pl.BlockSpec(memory_space=pltpu.SMEM),
            far_off,
            far_off,
            held,
            far_off,
            far_off,
        ],
        out_specs=(far_off, far_off, held),
        scratch_shapes=[
            pltpu.VMEM((micro, tokens, width), jnp.bfloat16),
            pltpu.VMEM((width, inner), jnp.bfloat16),
            pltpu.VMEM((width, inner), jnp.bfloat16),
            pltpu.VMEM((inner, width), jnp.bfloat16),
            pltpu.VMEM((micro, tokens, 1), jnp.float32),
            pltpu.VMEM((micro, tokens, width), jnp.bfloat16),
            pltpu.VMEM((micro, tokens, width), jnp.bfloat16),
            pltpu.VMEM((tokens, width), jnp.bfloat16),
            pltpu.VMEM((chunk, width), jnp.float32),
            pltpu.VMEM((2, micro, 4 * tokens, inner), jnp.bfloat16),
            pltpu.VMEM((2, micro, width, tokens), jnp.bfloat16),
            pltpu.VMEM((2, micro, 2, share, 4 * tokens), jnp.bfloat16),
            pltpu.VMEM((2, 2, share, inner), jnp.float32),
            pltpu.VMEM((2, narrow, share, TILE), jnp.bfloat16),
            pltpu.VMEM((2, narrow, share, TILE), jnp.bfloat16),
            pltpu.VMEM((8, width), jnp.float32),
            pltpu.VMEM((peers, 1, width), jnp.float32),
            pltpu.SemaphoreType.DMA((4,)),
            pltpu.SemaphoreType.DMA((2, narrow)),
            pltpu.SemaphoreType.DMA((2, micro, CHUNKS, 3)),
            pltpu.SemaphoreType.DMA((2, micro, CHUNKS, 3)),
            pltpu.SemaphoreType.DMA((2, micro, peers, 2)),
            pltpu.SemaphoreType.DMA((2, micro, peers, 2)),
            pltpu.SemaphoreType.DMA((micro * CHUNKS,)),
            pltpu.SemaphoreType.DMA((micro * CHUNKS,)),
            pltpu.SemaphoreType.DMA((2, narrow)),
            pltpu.SemaphoreType.DMA((2, narrow)),
            pltpu.SemaphoreType.DMA((peers,)),
            pltpu.SemaphoreType.DMA((peers,)),
        ],
        compiler_params=pltpu.CompilerParams(
            collective_id=0, has_side_effects=True, vmem_limit_bytes=VMEM_BYTES
        ),
    )(slot_table, saved[0], cotangent, gain, value_weight[0], out_weight[0])
    return value_grad[None], out_grad[None], gain_grad


def fits(mesh, saved, cotangent, slot_table, gain, value_weight, out_weight):
    peers = mesh.shape["seq"]
    micro, tokens, width = cotangent.shape
    inner = value_weight.shape[2]
    share = width // peers
    held = 6 * width * inner + 2 * 2 * micro * 4 * tokens * (inner + 2 * share)
    held += 2 * micro * tokens * width * 5 + 6 * tokens * width
    held += share * inner * (4 * 4 + 4 * 2 + 4 * 2)
    return (
        peers == 8
        and tokens % LANES == 0
        and width % (3 * TILE) == 0
        and inner % (2 * TILE) == 0
        and width % (16 * peers) == 0
        and held < VMEM_BYTES - 4 * 1024 * 1024
    )


def on_device(mesh, *arrays):
    if fits(mesh, *arrays):
        return fused(mesh, *arrays)
    return per_device(*arrays)


def solution(mesh):
    in_specs = (
        P("section", None, "seq", None),
        P(None, "seq", None),
        P("section", None),
        P("section", None),
        P("section", None, None),
        P("section", None, None),
    )
    out_specs = (P("section", "seq", None), P("section", "seq", None), P("section", None))
    return jax.shard_map(
        functools.partial(on_device, mesh), mesh=mesh, in_specs=in_specs, out_specs=out_specs, check_vma=False
    )
```

```python
import functools

import jax
import jax.numpy as jnp
from jax import lax
from jax.experimental import pallas as pl
from jax.experimental.pallas import tpu as pltpu
from jax.sharding import PartitionSpec as P

EPSILON = 1e-06


def passed_along(value, axis, steps):
    count = lax.axis_size(axis)
    first, last = (max(0, -steps), min(count, count - steps))
    return lax.ppermute(value, axis, [(source, source + steps) for source in range(first, last)])


def normalize(inputs, gain_row):
    value_rows = inputs.astype(jnp.float32)
    inv_rms = lax.rsqrt(jnp.mean(value_rows * value_rows, axis=-1, keepdims=True) + EPSILON)
    unit_rows = value_rows * inv_rms
    return (unit_rows, inv_rms, (unit_rows * gain_row).astype(jnp.bfloat16))


def input_grads(inputs, grad_out, gain_row, w_value, w_out):
    unit_rows, inv_rms, normed = normalize(inputs, gain_row)
    grad_value = jnp.dot(grad_out, w_out, preferred_element_type=jnp.float32).astype(jnp.bfloat16)
    grad_normed = lax.dot_general(
        grad_value, w_value, (((1,), (1,)), ((), ())), preferred_element_type=jnp.float32
    )
    gain_term = jnp.sum(grad_normed * unit_rows, axis=0)
    grad_unit = grad_normed * gain_row
    grad_in = grad_out.astype(jnp.float32) + inv_rms * (
        grad_unit - unit_rows * jnp.mean(grad_unit * unit_rows, axis=-1, keepdims=True)
    )
    return (grad_in.astype(jnp.bfloat16), grad_value, normed, gain_term)


def arrivals(
    step_index, sent, section_count, section_index, micro_count, cotangent, local_saved, slot_order
):
    if step_index > 0:
        incoming = passed_along(sent, "section", -1)
    else:
        incoming = sent
    micro_index = step_index - (section_count - 1 - section_index)
    active_now = jnp.logical_and(micro_index >= 0, micro_index < micro_count)
    clipped = jnp.clip(micro_index, 0, micro_count - 1)
    top_grad = lax.dynamic_index_in_dim(cotangent, clipped, 0, keepdims=False)
    grad_out = jnp.where(section_index == section_count - 1, top_grad, incoming)
    slot_index = lax.dynamic_index_in_dim(slot_order, clipped, 0, keepdims=False)
    inputs = lax.dynamic_index_in_dim(local_saved, slot_index, 0, keepdims=False)
    return (active_now, clipped, grad_out, inputs)


def per_device(saved, cotangent, slot_table, gain, value_weight, out_weight):
    section_count = lax.axis_size("section")
    section_index = lax.axis_index("section")
    micro_count = slot_table.shape[1]
    local_saved = saved[0]
    slot_order = slot_table[0]
    gain_row = gain[0]
    w_value = value_weight[0]
    w_out = out_weight[0]
    token_rows = cotangent.shape[1]
    model_width = w_value.shape[0]
    inner_width = w_value.shape[1]
    sent = jnp.zeros((token_rows, model_width), jnp.bfloat16)
    gain_acc = jnp.zeros((model_width,), jnp.float32)
    out_stash = jnp.zeros((micro_count, token_rows, model_width), jnp.bfloat16)
    value_stash = jnp.zeros((micro_count, token_rows, inner_width), jnp.bfloat16)
    for step_index in range(micro_count + section_count - 1):
        active_now, clipped, grad_out, inputs = arrivals(
            step_index,
            sent,
            section_count,
            section_index,
            micro_count,
            cotangent,
            local_saved,
            slot_order,
        )

        def working(carried):
            grad_in, grad_value, normed, gain_term = input_grads(
                inputs, grad_out, gain_row, w_value, w_out
            )
            new_out = lax.dynamic_update_index_in_dim(carried[2], grad_out, clipped, 0)
            new_value = lax.dynamic_update_index_in_dim(carried[3], grad_value, clipped, 0)
            return (grad_in, carried[1] + gain_term, new_out, new_value)

        def resting(carried):
            return carried

        sent, gain_acc, out_stash, value_stash = lax.cond(
            active_now, working, resting, (sent, gain_acc, out_stash, value_stash)
        )
    ordered = jnp.take(local_saved, slot_order, axis=0).reshape(
        micro_count * token_rows, model_width
    )
    unit_all, inv_all, normed_all = normalize(ordered, gain_row)
    values_all = jnp.dot(normed_all, w_value, preferred_element_type=jnp.float32).astype(
        jnp.bfloat16
    )
    grads_all = out_stash.reshape(micro_count * token_rows, model_width)
    grad_values = value_stash.reshape(micro_count * token_rows, inner_width)
    value_acc = lax.dot_general(
        normed_all, grad_values, (((0,), (0,)), ((), ())), preferred_element_type=jnp.float32
    )
    out_acc = lax.dot_general(
        grads_all, values_all, (((0,), (0,)), ((), ())), preferred_element_type=jnp.float32
    )
    value_grad, out_grad = (
        lax.psum_scatter(value_acc, "seq", scatter_dimension=0, tiled=True),
        lax.psum_scatter(out_acc, "seq", scatter_dimension=0, tiled=True),
    )
    gain_total = lax.psum(gain_acc, "seq")
    return (value_grad[None], out_grad[None], gain_total[None])


TILE = 256
LANES = 128
CHUNKS = 4
VMEM_BYTES = 50 * 1024 * 1024


def flipped(index, bits, count):
    total, unit = 0, 1
    while unit < count:
        total = total + ((index // unit + (bits // unit) % 2) % 2) * unit
        unit *= 2
    return total


def tile_at(index, size=TILE):
    return pl.ds(pl.multiple_of(index * size, size), size)


def fused_kernel(
    peers,
    sections,
    slot_ref,
    saved_hbm,
    cot_hbm,
    gain_ref,
    wv_hbm,
    wo_hbm,
    vg_ref,
    og_ref,
    gg_ref,
    saved_ref,
    wv_ref,
    wo_ref,
    wvt_ref,
    inv_buf,
    grad_buf,
    pass_buf,
    normed,
    gn,
    rows_gv,
    rows_v,
    turned,
    cols_all,
    acc,
    part_out,
    part_in,
    gain_part,
    gain_all,
    load_sem,
    wv_sem,
    gv_send,
    gv_chip,
    gv_pair,
    v_send,
    v_chip,
    v_pair,
    cols_send,
    cols_recv,
    down_send,
    down_recv,
    part_send,
    part_recv,
    gain_send,
    gain_recv,
):
    section = lax.axis_index("section")
    me = lax.axis_index("seq")
    micro, tokens, width = grad_buf.shape
    inner = wv_ref.shape[1]
    share = width // peers
    wide, narrow = width // TILE, inner // TILE
    third = width // 3
    chunk, half = tokens // CHUNKS, tokens // 2
    steps = micro * CHUNKS
    top = section == sections - 1
    near = (peers // 4, peers // 2)
    far = (peers // 2, peers // 4)

    def peer(bits):
        return {"seq": flipped(me, bits, peers)}

    def coordinate(device, bit):
        return (device // bit) % 2

    def place(kind, device):
        return coordinate(device, near[kind]) * 2 + device % 2

    def remote(source, target, send_sem, recv_sem, device):
        return pltpu.make_async_remote_copy(
            src_ref=source,
            dst_ref=target,
            send_sem=send_sem,
            recv_sem=recv_sem,
            device_id=device,
            device_id_type=pl.DeviceIdType.MESH,
        )

    def gv_copy(k, owner, recv_sem, bits):
        m, h = k // CHUNKS, k % CHUNKS
        spot = rows_gv.at[m, tile_at(place(0, owner) * CHUNKS + h, chunk)]
        return remote(spot, spot, gv_send.at[0], recv_sem, peer(bits))

    def gv_to_chip(k):
        return gv_copy(k, me, gv_chip.at[k], near[0])

    def gv_from_chip(k):
        return gv_copy(k, flipped(me, near[0], peers), gv_chip.at[k], near[0])

    def gv_to_core(k):
        return gv_copy(k, me, gv_pair.at[k // CHUNKS], 1)

    def gv_relay(k):
        return gv_copy(k, flipped(me, near[0], peers), gv_pair.at[k // CHUNKS], 1)

    def gv_pairs(m):
        spot = rows_gv.at[m, : 2 * tokens]
        return remote(spot, spot, gv_send.at[0], gv_pair.at[m], peer(1))

    def gv_all():
        spot = rows_gv.at[:, : 3 * tokens]
        return remote(spot, spot, gv_send.at[0], gv_pair.at[0], peer(1))

    def v_copy(m, owner, recv_sem, bits):
        spot = rows_v.at[m, :, tile_at(place(1, owner), half)]
        return remote(spot, spot, v_send.at[0], recv_sem, peer(bits))

    def v_to_chip(m):
        return v_copy(m, me, v_chip.at[m], near[1])

    def v_from_chip(m):
        return v_copy(m, flipped(me, near[1], peers), v_chip.at[m], near[1])

    def v_to_core(m):
        return v_copy(m, me, v_pair.at[m], 1)

    def v_relay(m):
        return v_copy(m, flipped(me, near[1], peers), v_pair.at[m], 1)

    def v_pairs(m):
        spot = rows_v.at[m, :, : 2 * half]
        return remote(spot, spot, v_send.at[0], v_pair.at[m], peer(1))

    def v_all():
        spot = rows_v.at[:, :, : 3 * half]
        return remote(spot, spot, v_send.at[0], v_pair.at[0], peer(1))

    def ways(kind):
        return (near[kind], near[kind] + 1, 1)

    def col_source(kind, m, part, target):
        if kind == 0:
            block = target + (part - coordinate(target, far[0])) * far[0]
        else:
            block = part * 4 + place(1, target)
        return turned.at[kind, m, tile_at(block, share)]

    def col_copy(kind, m, part, bits):
        return remote(
            col_source(kind, m, part, flipped(me, bits, peers)),
            cols_all.at[kind, m, part, :, tile_at(place(kind, me), tokens)],
            cols_send.at[kind],
            cols_recv.at[kind, m, part if kind == 1 else 0],
            peer(bits),
        )

    def send_cols(kind, m, parts):
        for bits in ways(kind):
            for part in parts:
                col_copy(kind, m, part, bits).start()
        for part in parts:
            cols_all[kind, m, part, :, tile_at(place(kind, me), tokens)] = col_source(
                kind, m, part, me
            )[...]

    def value_cols(m):
        spot = cols_all.at[0, m, :, :, : 3 * tokens]
        return remote(spot, spot, cols_send.at[0], cols_recv.at[0, m, 0], peer(1))

    def grad_cols(m, p):
        spot = cols_all.at[1, m, p, :, : 3 * tokens]
        return remote(spot, spot, cols_send.at[1], cols_recv.at[1, m, p], peer(1))

    def cols_sent(kind):
        spot = cols_all.at[kind, :, :, :, : 3 * tokens]
        return remote(spot, spot, cols_send.at[kind], cols_recv.at[kind, 0, 0], peer(1))

    def down_copy(k, target):
        spot = tile_at(k % CHUNKS, chunk)
        return remote(
            pass_buf.at[k // CHUNKS, spot],
            grad_buf.at[k // CHUNKS, spot],
            down_send.at[0],
            down_recv.at[k],
            {"section": target},
        )

    def part_copy(kind, j):
        return remote(
            part_out.at[kind, j],
            part_in.at[kind, j],
            part_send.at[kind],
            part_recv.at[kind, j],
            peer(far[kind]),
        )

    def gain_copy(bits):
        spot = gain_all.at[me]
        return remote(spot, spot, gain_send.at[0], gain_recv.at[0], peer(bits))

    def gains():
        spot = gain_all.at[: peers - 1]
        return remote(spot, spot, gain_send.at[0], gain_recv.at[0], peer(1))

    load_saved = pltpu.make_async_copy(saved_hbm, saved_ref, load_sem.at[0])
    load_wo = pltpu.make_async_copy(wo_hbm, wo_ref, load_sem.at[1])
    load_first = pltpu.make_async_copy(cot_hbm.at[0], grad_buf.at[0], load_sem.at[2])
    load_rest = pltpu.make_async_copy(cot_hbm.at[1:], grad_buf.at[1:], load_sem.at[3])

    def load_wv(j):
        rows = slice(j * third, (j + 1) * third)
        return pltpu.make_async_copy(wv_hbm.at[rows], wv_ref.at[rows], wv_sem.at[j])

    load_saved.start()

    @pl.when(top)
    def _():
        load_first.start()
        load_wo.start()
        for j in range(3):
            load_wv(j).start()
        load_rest.start()

    @pl.when(section < sections - 1)
    def _():
        for j in range(3):
            load_wv(j).start()
        load_wo.start()

    barrier = pltpu.get_barrier_semaphore()
    for bits in range(1, peers):
        pl.semaphore_signal(
            barrier, inc=1, device_id=peer(bits), device_id_type=pl.DeviceIdType.MESH
        )

    @pl.when(section > 0)
    def _():
        pl.semaphore_signal(
            barrier,
            inc=1,
            device_id={"section": section - 1},
            device_id_type=pl.DeviceIdType.MESH,
        )

    @pl.when(section < sections - 1)
    def _():
        pl.semaphore_signal(
            barrier,
            inc=1,
            device_id={"section": section + 1},
            device_id_type=pl.DeviceIdType.MESH,
        )

    gain_part[...] = jnp.zeros_like(gain_part)
    load_saved.wait()

    def scales(m, carry):
        slot = slot_ref[0, m]
        total = jnp.zeros((tokens, LANES), jnp.float32)
        for j in range(width // LANES):
            x = saved_ref[slot, :, j * LANES : (j + 1) * LANES].astype(jnp.float32)
            total = total + x * x
        total = jnp.sum(total, axis=1, keepdims=True)
        inv_buf[m] = lax.rsqrt(total / width + EPSILON)
        return carry

    lax.fori_loop(0, micro, scales, 0)

    pl.semaphore_wait(
        barrier,
        peers - 1
        + (section > 0).astype(jnp.int32)
        + (section < sections - 1).astype(jnp.int32),
    )

    @pl.when(top)
    def _():
        load_first.wait()
        load_wo.wait()

    @pl.when(section < sections - 1)
    def _():
        for j in range(3):
            load_wv(j).wait()

    def values(m):
        slot = slot_ref[0, m]
        inv = inv_buf[m]
        for j in range(wide):
            cols = slice(j * TILE, (j + 1) * TILE)
            x = saved_ref[slot, :, cols].astype(jnp.float32)
            n = (x * inv * gain_ref[:, cols]).astype(jnp.bfloat16)
            normed[:, cols] = n
            turned[0, m, cols] = n.T
        send_cols(0, m, (0, 1))
        result = jnp.dot(
            normed[...], wv_ref[...], preferred_element_type=jnp.float32
        ).astype(jnp.bfloat16)
        for p in range(2):
            rows_v[m, p, tile_at(place(1, me), half)] = result[p * half : (p + 1) * half]
        v_to_chip(m).start()
        v_to_core(m).start()

    def turn(m, p):
        block = width // 4
        for y in range(2):
            left, right = (
                grad_buf[m, tile_at(p, half), :].T[(2 * y + i) * block : (2 * y + i + 1) * block]
                for i in range(2)
            )
            turned[1, m, tile_at(p * 2 + y, block)] = jnp.concatenate([left, right], axis=1)

        @pl.when(p == 0)
        def _():
            send_cols(1, m, (0,))

        @pl.when(p == 1)
        def _():
            send_cols(1, m, (1,))

    def chain(k):
        m, h = k // CHUNKS, k % CHUNKS
        here = tile_at(h, chunk)
        slot = slot_ref[0, m]
        inv = inv_buf[m, here]
        mine = tile_at(place(0, me) * CHUNKS + h, chunk)
        turning = (h % (CHUNKS // 2)) == CHUNKS // 2 - 1

        @pl.when(section < sections - 1)
        def _():
            down_copy(k, section + 1).wait_recv()

        @pl.when(jnp.logical_and(section == 0, turning))
        def _():
            turn(m, h // (CHUNKS // 2))

        rows_gv[m, mine] = jnp.dot(
            grad_buf[m, here], wo_ref[...], preferred_element_type=jnp.float32
        ).astype(jnp.bfloat16)
        gv_to_chip(k).start()
        gv_to_core(k).start()

        def back(flip, first):
            grad_value = rows_gv[m, mine]
            total = jnp.zeros((chunk, LANES), jnp.float32)
            for j in range(3):
                cols = slice(j * third, (j + 1) * third)
                if flip:
                    if first:
                        load_wv(j).wait()
                    term = lax.dot_general(
                        grad_value,
                        wv_ref[cols],
                        (((1,), (1,)), ((), ())),
                        preferred_element_type=jnp.float32,
                    )
                else:
                    term = jnp.dot(
                        grad_value, wvt_ref[:, cols], preferred_element_type=jnp.float32
                    )
                unit = saved_ref[slot, here, cols].astype(jnp.float32) * inv
                grad_unit = term * gain_ref[:, cols]
                gn[:, cols] = grad_unit
                gain_part[:, cols] += jnp.sum(
                    (term * unit).reshape(chunk // 8, 8, third), axis=0
                )
                both = grad_unit * unit
                for i in range(third // LANES):
                    total = total + both[:, i * LANES : (i + 1) * LANES]
            return jnp.sum(total, axis=1, keepdims=True) / width

        def down(mean):
            pull = inv * inv * mean
            for j in range(wide):
                cols = slice(j * TILE, (j + 1) * TILE)
                pass_buf[m, here, cols] = (
                    grad_buf[m, here, cols].astype(jnp.float32)
                    + inv * gn[:, cols]
                    - saved_ref[slot, here, cols].astype(jnp.float32) * pull
                ).astype(jnp.bfloat16)
            down_copy(k, section - 1).start()

        @pl.when(jnp.logical_and(top, k == 0))
        def _():
            down(back(True, True))
            load_rest.wait()

        @pl.when(jnp.logical_and(top, k > 0))
        def _():
            down(back(True, False))

        @pl.when(section < sections - 1)
        def _():
            mean = back(False, False)

            @pl.when(section > 0)
            def _():
                down(mean)

        @pl.when(jnp.logical_and(section > 0, turning))
        def _():
            turn(m, h // (CHUNKS // 2))

    def relay_values():
        def one(m, carry):
            v_from_chip(m).wait_recv()
            v_relay(m).start()
            return carry

        lax.fori_loop(0, micro, one, 0)

    def relay_grads(k):
        gv_from_chip(k).wait_recv()
        gv_relay(k).start()

    def value_product(m):
        value_cols(m).wait_recv()
        gv_pairs(m).wait_recv()
        both = cols_all[0, m].reshape(2 * share, 4 * tokens)
        for j in range(inner // (2 * TILE)):
            cols = slice(j * 2 * TILE, (j + 1) * 2 * TILE)
            acc[0, :, :, cols] += jnp.dot(
                both, rows_gv[m, :, cols], preferred_element_type=jnp.float32
            ).reshape(2, share, 2 * TILE)

    def grad_lanes(m, p):
        packed = cols_all[1, m, p]
        return [
            jnp.concatenate(
                [
                    packed[:, (2 * place_of + b) * half : (2 * place_of + b + 1) * half]
                    for place_of in range(4)
                ],
                axis=1,
            )
            for b in range(2)
        ]

    def out_product(m, p):
        @pl.when(p == 0)
        def _():
            v_pairs(m).wait_recv()

        grad_cols(m, p).wait_recv()
        both = jnp.concatenate(grad_lanes(m, p), axis=0)
        for j in range(inner // (2 * TILE)):
            cols = slice(j * 2 * TILE, (j + 1) * 2 * TILE)
            acc[1, :, :, cols] += jnp.dot(
                both, rows_v[m, p, :, cols], preferred_element_type=jnp.float32
            ).reshape(2, share, 2 * TILE)

    def transpose_weights():
        def tile(j, carry):
            wvt_ref[:, tile_at(j)] = wv_ref[tile_at(j)].T
            return carry

        lax.fori_loop(0, wide, tile, 0)

    def stage(t, carry):
        at_top = top.astype(jnp.int32)
        lap, turn_of = t // (CHUNKS + 1), t % (CHUNKS + 1)
        chained = at_top * (turn_of < CHUNKS).astype(jnp.int32) + (1 - at_top) * (
            t >= micro
        ).astype(jnp.int32)
        k = at_top * (lap * CHUNKS + turn_of) + (1 - at_top) * (t - micro)
        m = at_top * lap + (1 - at_top) * t

        @pl.when(chained == 1)
        def _():
            @pl.when(jnp.logical_and(section < sections - 1, k == 0))
            def _():
                load_wo.wait()
                transpose_weights()

            @pl.when(jnp.logical_and(section == 0, k == 0))
            def _():
                acc[...] = jnp.zeros_like(acc)
                relay_values()

            chain(k)

            @pl.when(jnp.logical_and(section == 0, k > 0))
            def _():
                relay_grads(k - 1)

            @pl.when(
                jnp.logical_and(
                    section == 0, jnp.logical_and(k > CHUNKS, k % CHUNKS == 1)
                )
            )
            def _():
                value_product(k // CHUNKS - 1)

            @pl.when(
                jnp.logical_and(
                    section == 0,
                    jnp.logical_and(k > CHUNKS // 2, k % (CHUNKS // 2) == CHUNKS // 2 - 1),
                )
            )
            def _():
                unit = k // (CHUNKS // 2) - 1
                out_product(unit // 2, unit % 2)

        @pl.when(chained == 0)
        def _():
            values(m)

        return carry

    lax.fori_loop(0, steps + micro, stage, 0)
    gain_all[me] = jnp.sum(gain_part[...], axis=0, keepdims=True)
    for bits in range(1, peers):
        gain_copy(bits).start()

    @pl.when(section > 0)
    def _():
        acc[...] = jnp.zeros_like(acc)
        relay_values()

        def early(k, carry):
            relay_grads(k)
            return carry

        lax.fori_loop(0, steps - 1, early, 0)

        def heavy(m, carry):
            value_product(m)
            return carry

        lax.fori_loop(0, micro - 1, heavy, 0)

        def light(unit, carry):
            out_product(unit // 2, unit % 2)
            return carry

        lax.fori_loop(0, 2 * micro - 1, light, 0)

    relay_grads(steps - 1)
    last = micro - 1
    mine = coordinate(me, far[1])
    grad_cols(last, 1).wait_recv()
    lanes = grad_lanes(last, 1)
    give = jnp.where(mine == 0, lanes[1], lanes[0])
    keep = jnp.where(mine == 0, lanes[0], lanes[1])
    for j in range(narrow):
        cols = slice(j * TILE, (j + 1) * TILE)
        part_out[1, j] = (
            acc[1, 1 - mine, :, cols]
            + jnp.dot(give, rows_v[last, 1, :, cols], preferred_element_type=jnp.float32)
        ).astype(jnp.bfloat16)
        part_copy(1, j).start()

    side = coordinate(me, far[0])
    value_cols(last).wait_recv()
    gv_pairs(last).wait_recv()
    for j in range(narrow):
        cols = slice(j * TILE, (j + 1) * TILE)
        part_out[0, j] = (
            acc[0, 1 - side, :, cols]
            + jnp.dot(
                cols_all[0, last, 1 - side],
                rows_gv[last, :, cols],
                preferred_element_type=jnp.float32,
            )
        ).astype(jnp.bfloat16)
        part_copy(0, j).start()

    for j in range(narrow):
        cols = slice(j * TILE, (j + 1) * TILE)
        acc[1, mine, :, cols] += jnp.dot(
            keep, rows_v[last, 1, :, cols], preferred_element_type=jnp.float32
        )
        acc[0, side, :, cols] += jnp.dot(
            cols_all[0, last, side], rows_gv[last, :, cols], preferred_element_type=jnp.float32
        )

    gains().wait_recv()
    gained = gain_all[0]
    for owner in range(1, peers):
        gained = gained + gain_all[owner]
    gg_ref[...] = gained
    gv_all().wait_send()
    v_all().wait_send()
    for kind in (0, 1):
        cols_sent(kind).wait_send()

    @pl.when(section > 0)
    def _():
        remote(
            pass_buf, grad_buf, down_send.at[0], down_recv.at[0], {"section": section - 1}
        ).wait_send()

    gains().wait_send()
    for j in range(narrow):
        cols = slice(j * TILE, (j + 1) * TILE)
        for kind, row, out_ref in ((1, mine, og_ref), (0, side, vg_ref)):
            part_copy(kind, j).wait_recv()
            out_ref[:, cols] = acc[kind, row, :, cols] + part_in[kind, j].astype(jnp.float32)

    for kind in (0, 1):
        remote(
            part_out.at[kind], part_in.at[kind], part_send.at[kind], part_recv.at[kind, 0], peer(1)
        ).wait_send()


def fused(mesh, saved, cotangent, slot_table, gain, value_weight, out_weight):
    peers, sections = mesh.shape["seq"], mesh.shape["section"]
    micro, tokens, width = cotangent.shape
    inner = value_weight.shape[2]
    share = width // peers
    narrow = inner // TILE
    chunk = tokens // CHUNKS
    steps = micro * CHUNKS
    held = pl.BlockSpec(memory_space=pltpu.VMEM)
    far_off = pl.BlockSpec(memory_space=pl.ANY)
    value_grad, out_grad, gain_grad = pl.pallas_call(
        functools.partial(fused_kernel, peers, sections),
        out_shape=(
            jax.ShapeDtypeStruct((share, inner), jnp.float32),
            jax.ShapeDtypeStruct((share, inner), jnp.float32),
            jax.ShapeDtypeStruct((1, width), jnp.float32),
        ),
        in_specs=[
            pl.BlockSpec(memory_space=pltpu.SMEM),
            far_off,
            far_off,
            held,
            far_off,
            far_off,
        ],
        out_specs=(held, held, held),
        scratch_shapes=[
            pltpu.VMEM((micro, tokens, width), jnp.bfloat16),
            pltpu.VMEM((width, inner), jnp.bfloat16),
            pltpu.VMEM((width, inner), jnp.bfloat16),
            pltpu.VMEM((inner, width), jnp.bfloat16),
            pltpu.VMEM((micro, tokens, 1), jnp.float32),
            pltpu.VMEM((micro, tokens, width), jnp.bfloat16),
            pltpu.VMEM((micro, tokens, width), jnp.bfloat16),
            pltpu.VMEM((tokens, width), jnp.bfloat16),
            pltpu.VMEM((chunk, width), jnp.float32),
            pltpu.VMEM((micro, 4 * tokens, inner), jnp.bfloat16),
            pltpu.VMEM((micro, 2, 2 * tokens, inner), jnp.bfloat16),
            pltpu.VMEM((2, micro, width, tokens), jnp.bfloat16),
            pltpu.VMEM((2, micro, 2, share, 4 * tokens), jnp.bfloat16),
            pltpu.VMEM((2, 2, share, inner), jnp.float32),
            pltpu.VMEM((2, narrow, share, TILE), jnp.bfloat16),
            pltpu.VMEM((2, narrow, share, TILE), jnp.bfloat16),
            pltpu.VMEM((8, width), jnp.float32),
            pltpu.VMEM((peers, 1, width), jnp.float32),
            pltpu.SemaphoreType.DMA((4,)),
            pltpu.SemaphoreType.DMA((3,)),
            pltpu.SemaphoreType.DMA((1,)),
            pltpu.SemaphoreType.DMA((steps,)),
            pltpu.SemaphoreType.DMA((micro,)),
            pltpu.SemaphoreType.DMA((1,)),
            pltpu.SemaphoreType.DMA((micro,)),
            pltpu.SemaphoreType.DMA((micro,)),
            pltpu.SemaphoreType.DMA((2,)),
            pltpu.SemaphoreType.DMA((2, micro, 2)),
            pltpu.SemaphoreType.DMA((1,)),
            pltpu.SemaphoreType.DMA((steps,)),
            pltpu.SemaphoreType.DMA((2,)),
            pltpu.SemaphoreType.DMA((2, narrow)),
            pltpu.SemaphoreType.DMA((1,)),
            pltpu.SemaphoreType.DMA((1,)),
        ],
        compiler_params=pltpu.CompilerParams(
            collective_id=0, has_side_effects=True, vmem_limit_bytes=VMEM_BYTES
        ),
    )(slot_table, saved[0], cotangent, gain, value_weight[0], out_weight[0])
    return value_grad[None], out_grad[None], gain_grad


def fits(mesh, saved, cotangent, slot_table, gain, value_weight, out_weight):
    peers = mesh.shape["seq"]
    micro, tokens, width = cotangent.shape
    inner = value_weight.shape[2]
    share = width // peers
    held = 6 * width * inner + 2 * 2 * micro * 4 * tokens * (inner + 2 * share)
    held += 2 * micro * tokens * width * 5 + 6 * tokens * width
    held += share * inner * (4 * 4 + 4 * 2 + 4 * 2)
    return (
        peers == 8
        and micro > 1
        and tokens == LANES
        and width % (3 * TILE) == 0
        and inner % (2 * TILE) == 0
        and width % (16 * peers) == 0
        and held < VMEM_BYTES - 2 * 1024 * 1024
    )


def on_device(mesh, *arrays):
    if fits(mesh, *arrays):
        return fused(mesh, *arrays)
    return per_device(*arrays)


def solution(mesh):
    in_specs = (
        P("section", None, "seq", None),
        P(None, "seq", None),
        P("section", None),
        P("section", None),
        P("section", None, None),
        P("section", None, None),
    )
    out_specs = (P("section", "seq", None), P("section", "seq", None), P("section", None))
    return jax.shard_map(
        functools.partial(on_device, mesh), mesh=mesh, in_specs=in_specs, out_specs=out_specs, check_vma=False
    )
```

```python
import functools

import jax
import jax.numpy as jnp
from jax import lax
from jax.experimental import pallas as pl
from jax.experimental.pallas import tpu as pltpu
from jax.sharding import PartitionSpec as P

EPSILON = 1e-06


def passed_along(value, axis, steps):
    count = lax.axis_size(axis)
    first, last = (max(0, -steps), min(count, count - steps))
    return lax.ppermute(value, axis, [(source, source + steps) for source in range(first, last)])


def normalize(inputs, gain_row):
    value_rows = inputs.astype(jnp.float32)
    inv_rms = lax.rsqrt(jnp.mean(value_rows * value_rows, axis=-1, keepdims=True) + EPSILON)
    unit_rows = value_rows * inv_rms
    return (unit_rows, inv_rms, (unit_rows * gain_row).astype(jnp.bfloat16))


def input_grads(inputs, grad_out, gain_row, w_value, w_out):
    unit_rows, inv_rms, normed = normalize(inputs, gain_row)
    grad_value = jnp.dot(grad_out, w_out, preferred_element_type=jnp.float32).astype(jnp.bfloat16)
    grad_normed = lax.dot_general(
        grad_value, w_value, (((1,), (1,)), ((), ())), preferred_element_type=jnp.float32
    )
    gain_term = jnp.sum(grad_normed * unit_rows, axis=0)
    grad_unit = grad_normed * gain_row
    grad_in = grad_out.astype(jnp.float32) + inv_rms * (
        grad_unit - unit_rows * jnp.mean(grad_unit * unit_rows, axis=-1, keepdims=True)
    )
    return (grad_in.astype(jnp.bfloat16), grad_value, normed, gain_term)


def arrivals(
    step_index, sent, section_count, section_index, micro_count, cotangent, local_saved, slot_order
):
    if step_index > 0:
        incoming = passed_along(sent, "section", -1)
    else:
        incoming = sent
    micro_index = step_index - (section_count - 1 - section_index)
    active_now = jnp.logical_and(micro_index >= 0, micro_index < micro_count)
    clipped = jnp.clip(micro_index, 0, micro_count - 1)
    top_grad = lax.dynamic_index_in_dim(cotangent, clipped, 0, keepdims=False)
    grad_out = jnp.where(section_index == section_count - 1, top_grad, incoming)
    slot_index = lax.dynamic_index_in_dim(slot_order, clipped, 0, keepdims=False)
    inputs = lax.dynamic_index_in_dim(local_saved, slot_index, 0, keepdims=False)
    return (active_now, clipped, grad_out, inputs)


def per_device(saved, cotangent, slot_table, gain, value_weight, out_weight):
    section_count = lax.axis_size("section")
    section_index = lax.axis_index("section")
    micro_count = slot_table.shape[1]
    local_saved = saved[0]
    slot_order = slot_table[0]
    gain_row = gain[0]
    w_value = value_weight[0]
    w_out = out_weight[0]
    token_rows = cotangent.shape[1]
    model_width = w_value.shape[0]
    inner_width = w_value.shape[1]
    sent = jnp.zeros((token_rows, model_width), jnp.bfloat16)
    gain_acc = jnp.zeros((model_width,), jnp.float32)
    out_stash = jnp.zeros((micro_count, token_rows, model_width), jnp.bfloat16)
    value_stash = jnp.zeros((micro_count, token_rows, inner_width), jnp.bfloat16)
    for step_index in range(micro_count + section_count - 1):
        active_now, clipped, grad_out, inputs = arrivals(
            step_index,
            sent,
            section_count,
            section_index,
            micro_count,
            cotangent,
            local_saved,
            slot_order,
        )

        def working(carried):
            grad_in, grad_value, normed, gain_term = input_grads(
                inputs, grad_out, gain_row, w_value, w_out
            )
            new_out = lax.dynamic_update_index_in_dim(carried[2], grad_out, clipped, 0)
            new_value = lax.dynamic_update_index_in_dim(carried[3], grad_value, clipped, 0)
            return (grad_in, carried[1] + gain_term, new_out, new_value)

        def resting(carried):
            return carried

        sent, gain_acc, out_stash, value_stash = lax.cond(
            active_now, working, resting, (sent, gain_acc, out_stash, value_stash)
        )
    ordered = jnp.take(local_saved, slot_order, axis=0).reshape(
        micro_count * token_rows, model_width
    )
    unit_all, inv_all, normed_all = normalize(ordered, gain_row)
    values_all = jnp.dot(normed_all, w_value, preferred_element_type=jnp.float32).astype(
        jnp.bfloat16
    )
    grads_all = out_stash.reshape(micro_count * token_rows, model_width)
    grad_values = value_stash.reshape(micro_count * token_rows, inner_width)
    value_acc = lax.dot_general(
        normed_all, grad_values, (((0,), (0,)), ((), ())), preferred_element_type=jnp.float32
    )
    out_acc = lax.dot_general(
        grads_all, values_all, (((0,), (0,)), ((), ())), preferred_element_type=jnp.float32
    )
    value_grad, out_grad = (
        lax.psum_scatter(value_acc, "seq", scatter_dimension=0, tiled=True),
        lax.psum_scatter(out_acc, "seq", scatter_dimension=0, tiled=True),
    )
    gain_total = lax.psum(gain_acc, "seq")
    return (value_grad[None], out_grad[None], gain_total[None])


TILE = 256
LANES = 128
CHUNKS = 4
VMEM_BYTES = 50 * 1024 * 1024


def flipped(index, bits, count):
    total, unit = 0, 1
    while unit < count:
        total = total + ((index // unit + (bits // unit) % 2) % 2) * unit
        unit *= 2
    return total


def tile_at(index, size=TILE):
    return pl.ds(pl.multiple_of(index * size, size), size)


def fused_kernel(
    peers,
    sections,
    slot_ref,
    saved_hbm,
    cot_hbm,
    gain_ref,
    wv_hbm,
    wo_hbm,
    vg_ref,
    og_ref,
    gg_ref,
    saved_ref,
    wv_ref,
    wo_ref,
    wvt_ref,
    inv_buf,
    grad_buf,
    pass_buf,
    normed,
    gn,
    rows_gv,
    rows_v,
    turned,
    cols_all,
    acc,
    part_out,
    part_in,
    gain_part,
    gain_all,
    load_sem,
    wv_sem,
    gv_send,
    gv_chip,
    gv_pair,
    v_send,
    v_chip,
    v_pair,
    cols_send,
    cols_recv,
    down_send,
    down_recv,
    part_send,
    part_recv,
    gain_send,
    gain_recv,
):
    section = lax.axis_index("section")
    me = lax.axis_index("seq")
    micro, tokens, width = grad_buf.shape
    inner = wv_ref.shape[1]
    share = width // peers
    wide, narrow = width // TILE, inner // TILE
    third = width // 3
    chunk, half = tokens // CHUNKS, tokens // 2
    steps = micro * CHUNKS
    top = section == sections - 1
    near = (peers // 4, peers // 2)
    far = (peers // 2, peers // 4)

    def peer(bits):
        return {"seq": flipped(me, bits, peers)}

    def coordinate(device, bit):
        return (device // bit) % 2

    def place(kind, device):
        return coordinate(device, near[kind]) * 2 + device % 2

    def remote(source, target, send_sem, recv_sem, device):
        return pltpu.make_async_remote_copy(
            src_ref=source,
            dst_ref=target,
            send_sem=send_sem,
            recv_sem=recv_sem,
            device_id=device,
            device_id_type=pl.DeviceIdType.MESH,
        )

    def gv_copy(k, owner, recv_sem, bits):
        m, h = k // CHUNKS, k % CHUNKS
        spot = rows_gv.at[m, tile_at(place(0, owner) * CHUNKS + h, chunk)]
        return remote(spot, spot, gv_send.at[0], recv_sem, peer(bits))

    def gv_to_chip(k):
        return gv_copy(k, me, gv_chip.at[k], near[0])

    def gv_from_chip(k):
        return gv_copy(k, flipped(me, near[0], peers), gv_chip.at[k], near[0])

    def gv_to_core(k):
        return gv_copy(k, me, gv_pair.at[k // CHUNKS], 1)

    def gv_relay(k):
        return gv_copy(k, flipped(me, near[0], peers), gv_pair.at[k // CHUNKS], 1)

    def gv_pairs(m):
        spot = rows_gv.at[m, : 2 * tokens]
        return remote(spot, spot, gv_send.at[0], gv_pair.at[m], peer(1))

    def gv_all():
        spot = rows_gv.at[:, : 3 * tokens]
        return remote(spot, spot, gv_send.at[0], gv_pair.at[0], peer(1))

    def v_copy(m, owner, recv_sem, bits):
        spot = rows_v.at[m, :, tile_at(place(1, owner), half)]
        return remote(spot, spot, v_send.at[0], recv_sem, peer(bits))

    def v_to_chip(m):
        return v_copy(m, me, v_chip.at[m], near[1])

    def v_from_chip(m):
        return v_copy(m, flipped(me, near[1], peers), v_chip.at[m], near[1])

    def v_to_core(m):
        return v_copy(m, me, v_pair.at[m], 1)

    def v_relay(m):
        return v_copy(m, flipped(me, near[1], peers), v_pair.at[m], 1)

    def v_pairs(m):
        spot = rows_v.at[m, :, : 2 * half]
        return remote(spot, spot, v_send.at[0], v_pair.at[m], peer(1))

    def v_all():
        spot = rows_v.at[:, :, : 3 * half]
        return remote(spot, spot, v_send.at[0], v_pair.at[0], peer(1))

    def ways(kind):
        return (near[kind], near[kind] + 1, 1)

    def col_source(kind, m, part, target):
        if kind == 0:
            block = target + (part - coordinate(target, far[0])) * far[0]
        else:
            block = part * 4 + place(1, target)
        return turned.at[kind, m, tile_at(block, share)]

    def col_copy(kind, m, part, bits):
        return remote(
            col_source(kind, m, part, flipped(me, bits, peers)),
            cols_all.at[kind, m, part, :, tile_at(place(kind, me), tokens)],
            cols_send.at[kind],
            cols_recv.at[kind, m, part if kind == 1 else 0],
            peer(bits),
        )

    def send_cols(kind, m, parts):
        for bits in ways(kind):
            for part in parts:
                col_copy(kind, m, part, bits).start()
        for part in parts:
            cols_all[kind, m, part, :, tile_at(place(kind, me), tokens)] = col_source(
                kind, m, part, me
            )[...]

    def value_cols(m):
        spot = cols_all.at[0, m, :, :, : 3 * tokens]
        return remote(spot, spot, cols_send.at[0], cols_recv.at[0, m, 0], peer(1))

    def grad_cols(m, p):
        spot = cols_all.at[1, m, p, :, : 3 * tokens]
        return remote(spot, spot, cols_send.at[1], cols_recv.at[1, m, p], peer(1))

    def cols_sent(kind):
        spot = cols_all.at[kind, :, :, :, : 3 * tokens]
        return remote(spot, spot, cols_send.at[kind], cols_recv.at[kind, 0, 0], peer(1))

    def down_copy(k, g, target):
        spot, cols = tile_at(k % CHUNKS, chunk), slice(g * third, (g + 1) * third)
        return remote(
            pass_buf.at[k // CHUNKS, spot, cols],
            grad_buf.at[k // CHUNKS, spot, cols],
            down_send.at[0],
            down_recv.at[k, g],
            {"section": target},
        )

    def part_copy(kind, j):
        return remote(
            part_out.at[kind, j],
            part_in.at[kind, j],
            part_send.at[kind],
            part_recv.at[kind, j],
            peer(far[kind]),
        )

    def gain_copy(bits):
        spot = gain_all.at[me]
        return remote(spot, spot, gain_send.at[0], gain_recv.at[0], peer(bits))

    def gains():
        spot = gain_all.at[: peers - 1]
        return remote(spot, spot, gain_send.at[0], gain_recv.at[0], peer(1))

    load_saved = pltpu.make_async_copy(saved_hbm, saved_ref, load_sem.at[0])
    load_wo = pltpu.make_async_copy(wo_hbm, wo_ref, load_sem.at[1])
    load_first = pltpu.make_async_copy(cot_hbm.at[0], grad_buf.at[0], load_sem.at[2])
    load_rest = pltpu.make_async_copy(cot_hbm.at[1:], grad_buf.at[1:], load_sem.at[3])

    def load_wv(j):
        rows = slice(j * third, (j + 1) * third)
        return pltpu.make_async_copy(wv_hbm.at[rows], wv_ref.at[rows], wv_sem.at[j])

    load_saved.start()

    @pl.when(top)
    def _():
        load_first.start()
        load_wo.start()

    @pl.when(section < sections - 1)
    def _():
        for j in range(3):
            load_wv(j).start()
        load_wo.start()

    barrier = pltpu.get_barrier_semaphore()
    for bits in range(1, peers):
        pl.semaphore_signal(
            barrier, inc=1, device_id=peer(bits), device_id_type=pl.DeviceIdType.MESH
        )

    @pl.when(section > 0)
    def _():
        pl.semaphore_signal(
            barrier,
            inc=1,
            device_id={"section": section - 1},
            device_id_type=pl.DeviceIdType.MESH,
        )

    @pl.when(section < sections - 1)
    def _():
        pl.semaphore_signal(
            barrier,
            inc=1,
            device_id={"section": section + 1},
            device_id_type=pl.DeviceIdType.MESH,
        )

    gain_part[...] = jnp.zeros_like(gain_part)
    load_saved.wait()

    def scales(m, carry):
        slot = slot_ref[0, m]
        total = jnp.zeros((tokens, LANES), jnp.float32)
        for j in range(width // LANES):
            x = saved_ref[slot, :, j * LANES : (j + 1) * LANES].astype(jnp.float32)
            total = total + x * x
        total = jnp.sum(total, axis=1, keepdims=True)
        inv_buf[m] = lax.rsqrt(total / width + EPSILON)
        return carry

    lax.fori_loop(0, micro, scales, 0)

    @pl.when(top)
    def _():
        load_wv(0).start()
        load_wv(1).start()

    pl.semaphore_wait(
        barrier,
        peers - 1
        + (section > 0).astype(jnp.int32)
        + (section < sections - 1).astype(jnp.int32),
    )

    @pl.when(top)
    def _():
        load_first.wait()
        load_wo.wait()
        load_wv(2).start()
        load_rest.start()

    @pl.when(section < sections - 1)
    def _():
        for j in range(3):
            load_wv(j).wait()

    def values(m):
        slot = slot_ref[0, m]
        inv = inv_buf[m]
        for j in range(wide):
            cols = slice(j * TILE, (j + 1) * TILE)
            x = saved_ref[slot, :, cols].astype(jnp.float32)
            n = (x * inv * gain_ref[:, cols]).astype(jnp.bfloat16)
            normed[:, cols] = n
            turned[0, m, cols] = n.T
        send_cols(0, m, (0, 1))
        result = jnp.dot(
            normed[...], wv_ref[...], preferred_element_type=jnp.float32
        ).astype(jnp.bfloat16)
        for p in range(2):
            rows_v[m, p, tile_at(place(1, me), half)] = result[p * half : (p + 1) * half]
        v_to_chip(m).start()
        v_to_core(m).start()

    def turn(m, p):
        block = width // 4
        for y in range(2):
            left, right = (
                grad_buf[m, tile_at(p, half), :].T[(2 * y + i) * block : (2 * y + i + 1) * block]
                for i in range(2)
            )
            turned[1, m, tile_at(p * 2 + y, block)] = jnp.concatenate([left, right], axis=1)

        @pl.when(p == 0)
        def _():
            send_cols(1, m, (0,))

        @pl.when(p == 1)
        def _():
            send_cols(1, m, (1,))

    def dispatch(k, count, grad_value):
        m, h = k // CHUNKS, k % CHUNKS
        spot = place(0, me) * CHUNKS + h
        for i in range(count):
            rows_gv[m, tile_at(spot + i, chunk)] = grad_value[i * chunk : (i + 1) * chunk].astype(
                jnp.bfloat16
            )
        for i in range(count):
            gv_to_chip(k + i).start()
            gv_to_core(k + i).start()

    def whole(k, count, first):
        m, h = k // CHUNKS, k % CHUNKS
        rows = count * chunk
        here = tile_at(h // count, rows)
        slot = slot_ref[0, m]
        inv = inv_buf[m, here]
        dispatch(
            k,
            count,
            jnp.dot(grad_buf[m, here], wo_ref[...], preferred_element_type=jnp.float32),
        )
        grad_value = rows_gv[m, tile_at((place(0, me) * CHUNKS + h) // count, rows)]
        total = jnp.zeros((rows, LANES), jnp.float32)
        for j in range(3):
            cols = slice(j * third, (j + 1) * third)
            if first:
                load_wv(j).wait()
            term = lax.dot_general(
                grad_value,
                wv_ref[cols],
                (((1,), (1,)), ((), ())),
                preferred_element_type=jnp.float32,
            )
            unit = saved_ref[slot, here, cols].astype(jnp.float32) * inv
            grad_unit = term * gain_ref[:, cols]
            gn[:rows, cols] = grad_unit
            gain_part[:, cols] += jnp.sum((term * unit).reshape(rows // 8, 8, third), axis=0)
            both = grad_unit * unit
            for i in range(third // LANES):
                total = total + both[:, i * LANES : (i + 1) * LANES]
        pull = inv * inv * (jnp.sum(total, axis=1, keepdims=True) / width)
        for j in range(3):
            cols = slice(j * third, (j + 1) * third)
            pass_buf[m, here, cols] = (
                grad_buf[m, here, cols].astype(jnp.float32)
                + inv * gn[:rows, cols]
                - saved_ref[slot, here, cols].astype(jnp.float32) * pull
            ).astype(jnp.bfloat16)
        for i in range(count):
            for j in range(3):
                down_copy(k + i, j, section - 1).start()

    def chain(k):
        m, h = k // CHUNKS, k % CHUNKS
        here = tile_at(h, chunk)
        slot = slot_ref[0, m]
        inv = inv_buf[m, here]
        mine = tile_at(place(0, me) * CHUNKS + h, chunk)
        turning = (h % (CHUNKS // 2)) == CHUNKS // 2 - 1
        total = jnp.zeros((chunk, inner), jnp.float32)
        for g in range(3):
            cols = slice(g * third, (g + 1) * third)
            down_copy(k, g, section + 1).wait_recv()
            if g == 2:

                @pl.when(jnp.logical_and(section == 0, turning))
                def _():
                    turn(m, h // (CHUNKS // 2))

            total = total + jnp.dot(
                grad_buf[m, here, cols], wo_ref[cols], preferred_element_type=jnp.float32
            )
        dispatch(k, 1, total)

        @pl.when(section > 0)
        def _():
            grad_value = rows_gv[m, mine]
            own = place(1, me) * (CHUNKS // 2) + h % (CHUNKS // 2)
            value = rows_v[m, h // (CHUNKS // 2), tile_at(own, chunk)]
            dots = jnp.sum(
                grad_value.astype(jnp.float32) * value.astype(jnp.float32), axis=1, keepdims=True
            )
            pull = inv * inv * (dots / width)
            for j in range(3):
                cols = slice(j * third, (j + 1) * third)
                term = jnp.dot(grad_value, wvt_ref[:, cols], preferred_element_type=jnp.float32)
                x = saved_ref[slot, here, cols].astype(jnp.float32)
                pass_buf[m, here, cols] = (
                    grad_buf[m, here, cols].astype(jnp.float32)
                    + inv * (term * gain_ref[:, cols])
                    - x * pull
                ).astype(jnp.bfloat16)
                down_copy(k, j, section - 1).start()
                gain_part[:, cols] += jnp.sum(
                    (term * (x * inv)).reshape(chunk // 8, 8, third), axis=0
                )

        @pl.when(jnp.logical_and(section > 0, turning))
        def _():
            turn(m, h // (CHUNKS // 2))

    def gain_terms(m):
        slot = slot_ref[0, m]
        inv = inv_buf[m]
        grad_value = rows_gv[m, tile_at(place(0, me), tokens)]
        for j in range(3):
            cols = slice(j * third, (j + 1) * third)
            term = jnp.dot(grad_value, wvt_ref[:, cols], preferred_element_type=jnp.float32)
            unit = saved_ref[slot, :, cols].astype(jnp.float32) * inv
            gain_part[:, cols] += jnp.sum((term * unit).reshape(tokens // 8, 8, third), axis=0)

    def relay_values():
        def one(m, carry):
            v_from_chip(m).wait_recv()
            v_relay(m).start()
            return carry

        lax.fori_loop(0, micro, one, 0)

    def relay_grads(k):
        gv_from_chip(k).wait_recv()
        gv_relay(k).start()

    def value_product(m):
        value_cols(m).wait_recv()
        gv_pairs(m).wait_recv()
        both = cols_all[0, m].reshape(2 * share, 4 * tokens)
        for j in range(inner // (2 * TILE)):
            cols = slice(j * 2 * TILE, (j + 1) * 2 * TILE)
            acc[0, :, :, cols] += jnp.dot(
                both, rows_gv[m, :, cols], preferred_element_type=jnp.float32
            ).reshape(2, share, 2 * TILE)

    def grad_lanes(m, p):
        packed = cols_all[1, m, p]
        return [
            jnp.concatenate(
                [
                    packed[:, (2 * place_of + b) * half : (2 * place_of + b + 1) * half]
                    for place_of in range(4)
                ],
                axis=1,
            )
            for b in range(2)
        ]

    def out_product(m, p):
        @pl.when(p == 0)
        def _():
            v_pairs(m).wait_recv()

        grad_cols(m, p).wait_recv()
        both = jnp.concatenate(grad_lanes(m, p), axis=0)
        for j in range(inner // (2 * TILE)):
            cols = slice(j * 2 * TILE, (j + 1) * 2 * TILE)
            acc[1, :, :, cols] += jnp.dot(
                both, rows_v[m, p, :, cols], preferred_element_type=jnp.float32
            ).reshape(2, share, 2 * TILE)

    def transpose_weights():
        def tile(j, carry):
            wvt_ref[:, tile_at(j)] = wv_ref[tile_at(j)].T
            return carry

        lax.fori_loop(0, wide, tile, 0)

    @pl.when(top)
    def _():
        whole(0, 1, True)
        load_rest.wait()
        whole(1, 1, False)
        turn(0, 0)

        def pair(unit, carry):
            whole(unit * (CHUNKS // 2), CHUNKS // 2, False)
            turn(unit // 2, unit % 2)

            @pl.when(unit <= micro)
            def _():
                values(unit - 1)

            return carry

        lax.fori_loop(1, 2 * micro, pair, 0)

    def stage(t, carry):
        k = t - micro

        @pl.when(k >= 0)
        def _():
            @pl.when(k == 0)
            def _():
                load_wo.wait()
                transpose_weights()

            @pl.when(jnp.logical_and(section == 0, k == 0))
            def _():
                acc[...] = jnp.zeros_like(acc)
                relay_values()

            chain(k)

            @pl.when(jnp.logical_and(section == 0, k > 1))
            def _():
                relay_grads(k - 2)

            @pl.when(
                jnp.logical_and(
                    section == 0, jnp.logical_and(k > CHUNKS, k % CHUNKS == 2)
                )
            )
            def _():
                value_product(k // CHUNKS - 1)

            @pl.when(
                jnp.logical_and(
                    section == 0, jnp.logical_and(k >= CHUNKS, k % CHUNKS == 0)
                )
            )
            def _():
                gain_terms(k // CHUNKS - 1)

            @pl.when(
                jnp.logical_and(
                    section == 0,
                    jnp.logical_and(k > CHUNKS // 2, k % (CHUNKS // 2) == CHUNKS // 2 - 1),
                )
            )
            def _():
                unit = k // (CHUNKS // 2) - 1
                out_product(unit // 2, unit % 2)

        @pl.when(k < 0)
        def _():
            values(t)

        return carry

    @pl.when(section < sections - 1)
    def _():
        lax.fori_loop(0, steps + micro, stage, 0)

    @pl.when(section == 0)
    def _():
        relay_grads(steps - 2)
        gain_terms(micro - 1)

    gain_all[me] = jnp.sum(gain_part[...], axis=0, keepdims=True)
    for bits in range(1, peers):
        gain_copy(bits).start()

    @pl.when(section > 0)
    def _():
        acc[...] = jnp.zeros_like(acc)
        relay_values()

        def early(k, carry):
            relay_grads(k)
            return carry

        lax.fori_loop(0, steps - 1, early, 0)

        def heavy(m, carry):
            value_product(m)
            return carry

        lax.fori_loop(0, micro - 1, heavy, 0)

        def light(unit, carry):
            out_product(unit // 2, unit % 2)
            return carry

        lax.fori_loop(0, 2 * micro - 1, light, 0)

    relay_grads(steps - 1)
    last = micro - 1
    mine = coordinate(me, far[1])
    grad_cols(last, 1).wait_recv()
    lanes = grad_lanes(last, 1)
    give = jnp.where(mine == 0, lanes[1], lanes[0])
    keep = jnp.where(mine == 0, lanes[0], lanes[1])
    side = coordinate(me, far[0])
    value_cols(last).wait_recv()
    gv_pairs(last).wait_recv()
    for j in range(narrow):
        cols = slice(j * TILE, (j + 1) * TILE)
        part_out[1, j] = (
            acc[1, 1 - mine, :, cols]
            + jnp.dot(give, rows_v[last, 1, :, cols], preferred_element_type=jnp.float32)
        ).astype(jnp.bfloat16)
        part_copy(1, j).start()
        part_out[0, j] = (
            acc[0, 1 - side, :, cols]
            + jnp.dot(
                cols_all[0, last, 1 - side],
                rows_gv[last, :, cols],
                preferred_element_type=jnp.float32,
            )
        ).astype(jnp.bfloat16)
        part_copy(0, j).start()

    for j in range(narrow):
        cols = slice(j * TILE, (j + 1) * TILE)
        acc[1, mine, :, cols] += jnp.dot(
            keep, rows_v[last, 1, :, cols], preferred_element_type=jnp.float32
        )
        acc[0, side, :, cols] += jnp.dot(
            cols_all[0, last, side], rows_gv[last, :, cols], preferred_element_type=jnp.float32
        )

    gains().wait_recv()
    gained = gain_all[0]
    for owner in range(1, peers):
        gained = gained + gain_all[owner]
    gg_ref[...] = gained
    gv_all().wait_send()
    v_all().wait_send()
    for kind in (0, 1):
        cols_sent(kind).wait_send()

    @pl.when(section > 0)
    def _():
        remote(
            pass_buf, grad_buf, down_send.at[0], down_recv.at[0, 0], {"section": section - 1}
        ).wait_send()

    gains().wait_send()
    for j in range(narrow):
        cols = slice(j * TILE, (j + 1) * TILE)
        for kind, row, out_ref in ((1, mine, og_ref), (0, side, vg_ref)):
            part_copy(kind, j).wait_recv()
            out_ref[:, cols] = acc[kind, row, :, cols] + part_in[kind, j].astype(jnp.float32)

    for kind in (0, 1):
        remote(
            part_out.at[kind], part_in.at[kind], part_send.at[kind], part_recv.at[kind, 0], peer(1)
        ).wait_send()


def place_outputs(vg_ref, og_ref, gg_ref, vg_out, og_out, gg_out, sem):
    pairs = ((vg_ref, vg_out), (og_ref, og_out), (gg_ref, gg_out))
    copies = [
        pltpu.make_async_copy(source, target, sem.at[i])
        for i, (source, target) in enumerate(pairs)
    ]
    for copy in copies:
        copy.start()
    for copy in copies:
        copy.wait()


def fused(mesh, saved, cotangent, slot_table, gain, value_weight, out_weight):
    peers, sections = mesh.shape["seq"], mesh.shape["section"]
    micro, tokens, width = cotangent.shape
    inner = value_weight.shape[2]
    share = width // peers
    narrow = inner // TILE
    chunk = tokens // CHUNKS
    steps = micro * CHUNKS
    held = pl.BlockSpec(memory_space=pltpu.VMEM)
    far_off = pl.BlockSpec(memory_space=pl.ANY)
    value_grad, out_grad, gain_grad = pl.pallas_call(
        functools.partial(fused_kernel, peers, sections),
        out_shape=(
            jax.ShapeDtypeStruct((share, inner), jnp.float32),
            jax.ShapeDtypeStruct((share, inner), jnp.float32),
            jax.ShapeDtypeStruct((1, width), jnp.float32),
        ),
        in_specs=[
            pl.BlockSpec(memory_space=pltpu.SMEM),
            far_off,
            far_off,
            held,
            far_off,
            far_off,
        ],
        out_specs=(held, held, held),
        scratch_shapes=[
            pltpu.VMEM((micro, tokens, width), jnp.bfloat16),
            pltpu.VMEM((width, inner), jnp.bfloat16),
            pltpu.VMEM((width, inner), jnp.bfloat16),
            pltpu.VMEM((inner, width), jnp.bfloat16),
            pltpu.VMEM((micro, tokens, 1), jnp.float32),
            pltpu.VMEM((micro, tokens, width), jnp.bfloat16),
            pltpu.VMEM((micro, tokens, width), jnp.bfloat16),
            pltpu.VMEM((tokens, width), jnp.bfloat16),
            pltpu.VMEM((tokens // 2, width), jnp.float32),
            pltpu.VMEM((micro, 4 * tokens, inner), jnp.bfloat16),
            pltpu.VMEM((micro, 2, 2 * tokens, inner), jnp.bfloat16),
            pltpu.VMEM((2, micro, width, tokens), jnp.bfloat16),
            pltpu.VMEM((2, micro, 2, share, 4 * tokens), jnp.bfloat16),
            pltpu.VMEM((2, 2, share, inner), jnp.float32),
            pltpu.VMEM((2, narrow, share, TILE), jnp.bfloat16),
            pltpu.VMEM((2, narrow, share, TILE), jnp.bfloat16),
            pltpu.VMEM((8, width), jnp.float32),
            pltpu.VMEM((peers, 1, width), jnp.float32),
            pltpu.SemaphoreType.DMA((4,)),
            pltpu.SemaphoreType.DMA((3,)),
            pltpu.SemaphoreType.DMA((1,)),
            pltpu.SemaphoreType.DMA((steps,)),
            pltpu.SemaphoreType.DMA((micro,)),
            pltpu.SemaphoreType.DMA((1,)),
            pltpu.SemaphoreType.DMA((micro,)),
            pltpu.SemaphoreType.DMA((micro,)),
            pltpu.SemaphoreType.DMA((2,)),
            pltpu.SemaphoreType.DMA((2, micro, 2)),
            pltpu.SemaphoreType.DMA((1,)),
            pltpu.SemaphoreType.DMA((steps, 3)),
            pltpu.SemaphoreType.DMA((2,)),
            pltpu.SemaphoreType.DMA((2, narrow)),
            pltpu.SemaphoreType.DMA((1,)),
            pltpu.SemaphoreType.DMA((1,)),
        ],
        compiler_params=pltpu.CompilerParams(
            collective_id=0, has_side_effects=True, vmem_limit_bytes=VMEM_BYTES
        ),
    )(slot_table, saved[0], cotangent, gain, value_weight[0], out_weight[0])
    value_grad, out_grad, gain_grad = pl.pallas_call(
        place_outputs,
        out_shape=(
            jax.ShapeDtypeStruct((share, inner), jnp.float32),
            jax.ShapeDtypeStruct((share, inner), jnp.float32),
            jax.ShapeDtypeStruct((1, width), jnp.float32),
        ),
        in_specs=[far_off] * 3,
        out_specs=(far_off,) * 3,
        scratch_shapes=[pltpu.SemaphoreType.DMA((3,))],
        compiler_params=pltpu.CompilerParams(vmem_limit_bytes=8 * 1024 * 1024),
    )(value_grad, out_grad, gain_grad)
    return value_grad[None], out_grad[None], gain_grad


def fits(mesh, saved, cotangent, slot_table, gain, value_weight, out_weight):
    peers = mesh.shape["seq"]
    micro, tokens, width = cotangent.shape
    inner = value_weight.shape[2]
    share = width // peers
    held = 6 * width * inner + 2 * 2 * micro * 4 * tokens * (inner + 2 * share)
    held += 2 * micro * tokens * width * 5 + 6 * tokens * width
    held += share * inner * (4 * 4 + 4 * 2 + 4 * 2)
    return (
        peers == 8
        and micro > 1
        and tokens == LANES
        and width % (3 * TILE) == 0
        and inner % (2 * TILE) == 0
        and width % (16 * peers) == 0
        and held < VMEM_BYTES - 2 * 1024 * 1024
    )


def on_device(mesh, *arrays):
    if fits(mesh, *arrays):
        return fused(mesh, *arrays)
    return per_device(*arrays)


def solution(mesh):
    in_specs = (
        P("section", None, "seq", None),
        P(None, "seq", None),
        P("section", None),
        P("section", None),
        P("section", None, None),
        P("section", None, None),
    )
    out_specs = (P("section", "seq", None), P("section", "seq", None), P("section", None))
    return jax.shard_map(
        functools.partial(on_device, mesh), mesh=mesh, in_specs=in_specs, out_specs=out_specs, check_vma=False
    )
```

```python
import functools

import jax
import jax.numpy as jnp
from jax import lax
from jax.experimental import pallas as pl
from jax.experimental.pallas import tpu as pltpu
from jax.sharding import PartitionSpec as P

EPSILON = 1e-06


def passed_along(value, axis, steps):
    count = lax.axis_size(axis)
    first, last = (max(0, -steps), min(count, count - steps))
    return lax.ppermute(value, axis, [(source, source + steps) for source in range(first, last)])


def normalize(inputs, gain_row):
    value_rows = inputs.astype(jnp.float32)
    inv_rms = lax.rsqrt(jnp.mean(value_rows * value_rows, axis=-1, keepdims=True) + EPSILON)
    unit_rows = value_rows * inv_rms
    return (unit_rows, inv_rms, (unit_rows * gain_row).astype(jnp.bfloat16))


def input_grads(inputs, grad_out, gain_row, w_value, w_out):
    unit_rows, inv_rms, normed = normalize(inputs, gain_row)
    grad_value = jnp.dot(grad_out, w_out, preferred_element_type=jnp.float32).astype(jnp.bfloat16)
    grad_normed = lax.dot_general(
        grad_value, w_value, (((1,), (1,)), ((), ())), preferred_element_type=jnp.float32
    )
    gain_term = jnp.sum(grad_normed * unit_rows, axis=0)
    grad_unit = grad_normed * gain_row
    grad_in = grad_out.astype(jnp.float32) + inv_rms * (
        grad_unit - unit_rows * jnp.mean(grad_unit * unit_rows, axis=-1, keepdims=True)
    )
    return (grad_in.astype(jnp.bfloat16), grad_value, normed, gain_term)


def arrivals(
    step_index, sent, section_count, section_index, micro_count, cotangent, local_saved, slot_order
):
    if step_index > 0:
        incoming = passed_along(sent, "section", -1)
    else:
        incoming = sent
    micro_index = step_index - (section_count - 1 - section_index)
    active_now = jnp.logical_and(micro_index >= 0, micro_index < micro_count)
    clipped = jnp.clip(micro_index, 0, micro_count - 1)
    top_grad = lax.dynamic_index_in_dim(cotangent, clipped, 0, keepdims=False)
    grad_out = jnp.where(section_index == section_count - 1, top_grad, incoming)
    slot_index = lax.dynamic_index_in_dim(slot_order, clipped, 0, keepdims=False)
    inputs = lax.dynamic_index_in_dim(local_saved, slot_index, 0, keepdims=False)
    return (active_now, clipped, grad_out, inputs)


def per_device(saved, cotangent, slot_table, gain, value_weight, out_weight):
    section_count = lax.axis_size("section")
    section_index = lax.axis_index("section")
    micro_count = slot_table.shape[1]
    local_saved = saved[0]
    slot_order = slot_table[0]
    gain_row = gain[0]
    w_value = value_weight[0]
    w_out = out_weight[0]
    token_rows = cotangent.shape[1]
    model_width = w_value.shape[0]
    inner_width = w_value.shape[1]
    sent = jnp.zeros((token_rows, model_width), jnp.bfloat16)
    gain_acc = jnp.zeros((model_width,), jnp.float32)
    out_stash = jnp.zeros((micro_count, token_rows, model_width), jnp.bfloat16)
    value_stash = jnp.zeros((micro_count, token_rows, inner_width), jnp.bfloat16)
    for step_index in range(micro_count + section_count - 1):
        active_now, clipped, grad_out, inputs = arrivals(
            step_index,
            sent,
            section_count,
            section_index,
            micro_count,
            cotangent,
            local_saved,
            slot_order,
        )

        def working(carried):
            grad_in, grad_value, normed, gain_term = input_grads(
                inputs, grad_out, gain_row, w_value, w_out
            )
            new_out = lax.dynamic_update_index_in_dim(carried[2], grad_out, clipped, 0)
            new_value = lax.dynamic_update_index_in_dim(carried[3], grad_value, clipped, 0)
            return (grad_in, carried[1] + gain_term, new_out, new_value)

        def resting(carried):
            return carried

        sent, gain_acc, out_stash, value_stash = lax.cond(
            active_now, working, resting, (sent, gain_acc, out_stash, value_stash)
        )
    ordered = jnp.take(local_saved, slot_order, axis=0).reshape(
        micro_count * token_rows, model_width
    )
    unit_all, inv_all, normed_all = normalize(ordered, gain_row)
    values_all = jnp.dot(normed_all, w_value, preferred_element_type=jnp.float32).astype(
        jnp.bfloat16
    )
    grads_all = out_stash.reshape(micro_count * token_rows, model_width)
    grad_values = value_stash.reshape(micro_count * token_rows, inner_width)
    value_acc = lax.dot_general(
        normed_all, grad_values, (((0,), (0,)), ((), ())), preferred_element_type=jnp.float32
    )
    out_acc = lax.dot_general(
        grads_all, values_all, (((0,), (0,)), ((), ())), preferred_element_type=jnp.float32
    )
    value_grad, out_grad = (
        lax.psum_scatter(value_acc, "seq", scatter_dimension=0, tiled=True),
        lax.psum_scatter(out_acc, "seq", scatter_dimension=0, tiled=True),
    )
    gain_total = lax.psum(gain_acc, "seq")
    return (value_grad[None], out_grad[None], gain_total[None])


TILE = 256
LANES = 128
CHUNKS = 4
VMEM_BYTES = 50 * 1024 * 1024


def flipped(index, bits, count):
    total, unit = 0, 1
    while unit < count:
        total = total + ((index // unit + (bits // unit) % 2) % 2) * unit
        unit *= 2
    return total


def tile_at(index, size=TILE):
    return pl.ds(pl.multiple_of(index * size, size), size)


def fused_kernel(
    peers,
    sections,
    slot_hbm,
    saved_hbm,
    cot_hbm,
    gain_ref,
    wv_hbm,
    wo_hbm,
    vg_ref,
    og_ref,
    gg_ref,
    saved_ref,
    wv_ref,
    wo_ref,
    wvt_ref,
    inv_buf,
    grad_buf,
    pass_buf,
    normed,
    gn,
    rows_gv,
    rows_v,
    turned,
    cols_all,
    acc,
    part_out,
    part_in,
    gain_part,
    gain_all,
    slot_ref,
    load_sem,
    wv_sem,
    gv_send,
    gv_chip,
    gv_pair,
    v_send,
    v_chip,
    v_pair,
    cols_send,
    cols_recv,
    down_send,
    down_recv,
    part_send,
    part_recv,
    gain_send,
    gain_recv,
):
    section = lax.axis_index("section")
    me = lax.axis_index("seq")
    micro, tokens, width = grad_buf.shape
    inner = wv_ref.shape[1]
    share = width // peers
    wide, narrow = width // TILE, inner // TILE
    third = width // 3
    edges = [TILE * at for at in (0, wide // 3, wide - wide // 3, wide)]
    groups = [slice(low, high) for low, high in zip(edges[:-1], edges[1:])]
    chunk, half = tokens // CHUNKS, tokens // 2
    steps = micro * CHUNKS
    top = section == sections - 1
    near = (peers // 4, peers // 2)
    far = (peers // 2, peers // 4)

    def peer(bits):
        return {"seq": flipped(me, bits, peers)}

    def coordinate(device, bit):
        return (device // bit) % 2

    def place(kind, device):
        return coordinate(device, near[kind]) * 2 + device % 2

    def remote(source, target, send_sem, recv_sem, device):
        return pltpu.make_async_remote_copy(
            src_ref=source,
            dst_ref=target,
            send_sem=send_sem,
            recv_sem=recv_sem,
            device_id=device,
            device_id_type=pl.DeviceIdType.MESH,
        )

    def gv_copy(k, owner, recv_sem, bits):
        m, h = k // CHUNKS, k % CHUNKS
        spot = rows_gv.at[m, tile_at(place(0, owner) * CHUNKS + h, chunk)]
        return remote(spot, spot, gv_send.at[0], recv_sem, peer(bits))

    def gv_to_chip(k):
        return gv_copy(k, me, gv_chip.at[k], near[0])

    def gv_from_chip(k):
        return gv_copy(k, flipped(me, near[0], peers), gv_chip.at[k], near[0])

    def gv_to_core(k):
        return gv_copy(k, me, gv_pair.at[k // CHUNKS], 1)

    def gv_relay(k):
        return gv_copy(k, flipped(me, near[0], peers), gv_pair.at[k // CHUNKS], 1)

    def gv_pairs(m):
        spot = rows_gv.at[m, : 2 * tokens]
        return remote(spot, spot, gv_send.at[0], gv_pair.at[m], peer(1))

    def gv_all():
        spot = rows_gv.at[:, : 3 * tokens]
        return remote(spot, spot, gv_send.at[0], gv_pair.at[0], peer(1))

    def v_copy(m, owner, recv_sem, bits):
        spot = rows_v.at[m, :, tile_at(place(1, owner), half)]
        return remote(spot, spot, v_send.at[0], recv_sem, peer(bits))

    def v_to_chip(m):
        return v_copy(m, me, v_chip.at[m], near[1])

    def v_from_chip(m):
        return v_copy(m, flipped(me, near[1], peers), v_chip.at[m], near[1])

    def v_to_core(m):
        return v_copy(m, me, v_pair.at[m], 1)

    def v_relay(m):
        return v_copy(m, flipped(me, near[1], peers), v_pair.at[m], 1)

    def v_pairs(m):
        spot = rows_v.at[m, :, : 2 * half]
        return remote(spot, spot, v_send.at[0], v_pair.at[m], peer(1))

    def v_all():
        spot = rows_v.at[:, :, : 3 * half]
        return remote(spot, spot, v_send.at[0], v_pair.at[0], peer(1))

    def ways(kind):
        return (near[kind], near[kind] + 1, 1)

    def col_source(kind, m, part, target):
        if kind == 0:
            block = target + (part - coordinate(target, far[0])) * far[0]
        else:
            block = part * 4 + place(1, target)
        return turned.at[kind, m, tile_at(block, share)]

    def col_copy(kind, m, part, bits):
        return remote(
            col_source(kind, m, part, flipped(me, bits, peers)),
            cols_all.at[kind, m, part, :, tile_at(place(kind, me), tokens)],
            cols_send.at[kind],
            cols_recv.at[kind, m, part if kind == 1 else 0],
            peer(bits),
        )

    def send_cols(kind, m, parts):
        for bits in ways(kind):
            for part in parts:
                col_copy(kind, m, part, bits).start()
        for part in parts:
            cols_all[kind, m, part, :, tile_at(place(kind, me), tokens)] = col_source(
                kind, m, part, me
            )[...]

    def value_cols(m):
        spot = cols_all.at[0, m, :, :, : 3 * tokens]
        return remote(spot, spot, cols_send.at[0], cols_recv.at[0, m, 0], peer(1))

    def grad_cols(m, p):
        spot = cols_all.at[1, m, p, :, : 3 * tokens]
        return remote(spot, spot, cols_send.at[1], cols_recv.at[1, m, p], peer(1))

    def cols_sent(kind):
        spot = cols_all.at[kind, :, :, :, : 3 * tokens]
        return remote(spot, spot, cols_send.at[kind], cols_recv.at[kind, 0, 0], peer(1))

    def down_copy(k, g, target):
        spot, cols = tile_at(k % CHUNKS, chunk), groups[g]
        return remote(
            pass_buf.at[k // CHUNKS, spot, cols],
            grad_buf.at[k // CHUNKS, spot, cols],
            down_send.at[0],
            down_recv.at[k, g],
            {"section": target},
        )

    def part_copy(kind, j):
        return remote(
            part_out.at[kind, j],
            part_in.at[kind, j],
            part_send.at[kind],
            part_recv.at[kind, j],
            peer(far[kind]),
        )

    def gain_copy(bits):
        spot = gain_all.at[me]
        return remote(spot, spot, gain_send.at[0], gain_recv.at[0], peer(bits))

    def gains():
        spot = gain_all.at[: peers - 1]
        return remote(spot, spot, gain_send.at[0], gain_recv.at[0], peer(1))

    load_saved = pltpu.make_async_copy(saved_hbm, saved_ref, load_sem.at[0])
    load_slot = pltpu.make_async_copy(slot_hbm, slot_ref, load_sem.at[4])
    load_wo = pltpu.make_async_copy(wo_hbm, wo_ref, load_sem.at[1])
    load_first = pltpu.make_async_copy(cot_hbm.at[0], grad_buf.at[0], load_sem.at[2])
    load_rest = pltpu.make_async_copy(cot_hbm.at[1:], grad_buf.at[1:], load_sem.at[3])

    def load_wv(j):
        rows = slice(j * third, (j + 1) * third)
        return pltpu.make_async_copy(wv_hbm.at[rows], wv_ref.at[rows], wv_sem.at[j])

    @pl.when(top)
    def _():
        load_first.start()
        load_wo.start()

    @pl.when(section < sections - 1)
    def _():
        load_saved.start()
        for j in range(3):
            load_wv(j).start()
        load_wo.start()

    load_slot.start()
    barrier = pltpu.get_barrier_semaphore()
    for bits in range(1, peers):
        pl.semaphore_signal(
            barrier, inc=1, device_id=peer(bits), device_id_type=pl.DeviceIdType.MESH
        )

    @pl.when(section > 0)
    def _():
        pl.semaphore_signal(
            barrier,
            inc=1,
            device_id={"section": section - 1},
            device_id_type=pl.DeviceIdType.MESH,
        )

    @pl.when(section < sections - 1)
    def _():
        pl.semaphore_signal(
            barrier,
            inc=1,
            device_id={"section": section + 1},
            device_id_type=pl.DeviceIdType.MESH,
        )

    gain_part[...] = jnp.zeros_like(gain_part)

    @pl.when(top)
    def _():
        load_first.wait()
        load_saved.start()
        load_wv(0).start()

    @pl.when(section < sections - 1)
    def _():
        load_saved.wait()

    load_slot.wait()

    def scales(m, carry):
        slot = slot_ref[0, m]
        total = jnp.zeros((tokens, LANES), jnp.float32)
        for j in range(width // LANES):
            x = saved_ref[slot, :, j * LANES : (j + 1) * LANES].astype(jnp.float32)
            total = total + x * x
        total = jnp.sum(total, axis=1, keepdims=True)
        inv_buf[m] = lax.rsqrt(total / width + EPSILON)
        return carry

    @pl.when(section < sections - 1)
    def _():
        lax.fori_loop(0, micro, scales, 0)

    pl.semaphore_wait(
        barrier,
        peers - 1
        + (section > 0).astype(jnp.int32)
        + (section < sections - 1).astype(jnp.int32),
    )

    @pl.when(top)
    def _():
        load_wo.wait()
        load_wv(1).start()
        load_wv(2).start()
        load_rest.start()

    @pl.when(section < sections - 1)
    def _():
        for j in range(3):
            load_wv(j).wait()

    def values(m):
        slot = slot_ref[0, m]
        inv = inv_buf[m]
        for j in range(wide):
            cols = slice(j * TILE, (j + 1) * TILE)
            x = saved_ref[slot, :, cols].astype(jnp.float32)
            n = (x * inv * gain_ref[:, cols]).astype(jnp.bfloat16)
            normed[:, cols] = n
            turned[0, m, cols] = n.T
        send_cols(0, m, (0, 1))
        result = jnp.dot(
            normed[...], wv_ref[...], preferred_element_type=jnp.float32
        ).astype(jnp.bfloat16)
        for p in range(2):
            rows_v[m, p, tile_at(place(1, me), half)] = result[p * half : (p + 1) * half]
        v_to_chip(m).start()
        v_to_core(m).start()

    def turn(m, p):
        block = width // 4
        for y in range(2):
            left, right = (
                grad_buf[m, tile_at(p, half), :].T[(2 * y + i) * block : (2 * y + i + 1) * block]
                for i in range(2)
            )
            turned[1, m, tile_at(p * 2 + y, block)] = jnp.concatenate([left, right], axis=1)

        @pl.when(p == 0)
        def _():
            send_cols(1, m, (0,))

        @pl.when(p == 1)
        def _():
            send_cols(1, m, (1,))

    def dispatch(k, count, grad_value):
        m, h = k // CHUNKS, k % CHUNKS
        spot = place(0, me) * CHUNKS + h
        for i in range(count):
            rows_gv[m, tile_at(spot + i, chunk)] = grad_value[i * chunk : (i + 1) * chunk].astype(
                jnp.bfloat16
            )
        for i in range(count):
            gv_to_chip(k + i).start()
            gv_to_core(k + i).start()

    def whole(k, count, first):
        m, h = k // CHUNKS, k % CHUNKS
        rows = count * chunk
        here = tile_at(h // count, rows)
        slot = slot_ref[0, m]
        dispatch(
            k,
            count,
            jnp.dot(grad_buf[m, here], wo_ref[...], preferred_element_type=jnp.float32),
        )
        if first:
            load_saved.wait()
            scales(0, 0)
        inv = inv_buf[m, here]
        grad_value = rows_gv[m, tile_at((place(0, me) * CHUNKS + h) // count, rows)]
        total = jnp.zeros((rows, LANES), jnp.float32)
        for j in range(3):
            cols = slice(j * third, (j + 1) * third)
            if first:
                load_wv(j).wait()
            term = lax.dot_general(
                grad_value,
                wv_ref[cols],
                (((1,), (1,)), ((), ())),
                preferred_element_type=jnp.float32,
            )
            unit = saved_ref[slot, here, cols].astype(jnp.float32) * inv
            grad_unit = term * gain_ref[:, cols]
            gn[:rows, cols] = grad_unit
            gain_part[:, cols] += jnp.sum((term * unit).reshape(rows // 8, 8, third), axis=0)
            both = grad_unit * unit
            for i in range(third // LANES):
                total = total + both[:, i * LANES : (i + 1) * LANES]
        pull = inv * inv * (jnp.sum(total, axis=1, keepdims=True) / width)
        for j in range(3):
            cols = slice(j * third, (j + 1) * third)
            pass_buf[m, here, cols] = (
                grad_buf[m, here, cols].astype(jnp.float32)
                + inv * gn[:rows, cols]
                - saved_ref[slot, here, cols].astype(jnp.float32) * pull
            ).astype(jnp.bfloat16)
        for i in range(count):
            for g in range(len(groups)):
                down_copy(k + i, g, section - 1).start()

    def chain(k):
        m, h = k // CHUNKS, k % CHUNKS
        here = tile_at(h, chunk)
        slot = slot_ref[0, m]
        inv = inv_buf[m, here]
        mine = tile_at(place(0, me) * CHUNKS + h, chunk)
        turning = (h % (CHUNKS // 2)) == CHUNKS // 2 - 1
        total = jnp.zeros((chunk, inner), jnp.float32)
        for g, cols in enumerate(groups):
            down_copy(k, g, section + 1).wait_recv()
            if g == len(groups) - 1:

                @pl.when(jnp.logical_and(section == 0, turning))
                def _():
                    turn(m, h // (CHUNKS // 2))

            total = total + jnp.dot(
                grad_buf[m, here, cols], wo_ref[cols], preferred_element_type=jnp.float32
            )
        dispatch(k, 1, total)

        @pl.when(section > 0)
        def _():
            grad_value = rows_gv[m, mine]
            own = place(1, me) * (CHUNKS // 2) + h % (CHUNKS // 2)
            value = rows_v[m, h // (CHUNKS // 2), tile_at(own, chunk)]
            dots = jnp.sum(
                grad_value.astype(jnp.float32) * value.astype(jnp.float32), axis=1, keepdims=True
            )
            pull = inv * inv * (dots / width)
            for g, cols in enumerate(groups):
                term = jnp.dot(grad_value, wvt_ref[:, cols], preferred_element_type=jnp.float32)
                x = saved_ref[slot, here, cols].astype(jnp.float32)
                pass_buf[m, here, cols] = (
                    grad_buf[m, here, cols].astype(jnp.float32)
                    + inv * (term * gain_ref[:, cols])
                    - x * pull
                ).astype(jnp.bfloat16)
                down_copy(k, g, section - 1).start()
                gain_part[:, cols] += jnp.sum(
                    (term * (x * inv)).reshape(chunk // 8, 8, cols.stop - cols.start), axis=0
                )

        @pl.when(jnp.logical_and(section > 0, turning))
        def _():
            turn(m, h // (CHUNKS // 2))

    def gain_terms(m):
        slot = slot_ref[0, m]
        inv = inv_buf[m]
        grad_value = rows_gv[m, tile_at(place(0, me), tokens)]
        for j in range(3):
            cols = slice(j * third, (j + 1) * third)
            term = jnp.dot(grad_value, wvt_ref[:, cols], preferred_element_type=jnp.float32)
            unit = saved_ref[slot, :, cols].astype(jnp.float32) * inv
            gain_part[:, cols] += jnp.sum((term * unit).reshape(tokens // 8, 8, third), axis=0)

    def relay_values():
        def one(m, carry):
            v_from_chip(m).wait_recv()
            v_relay(m).start()
            return carry

        lax.fori_loop(0, micro, one, 0)

    def relay_grads(k):
        gv_from_chip(k).wait_recv()
        gv_relay(k).start()

    def value_product(m):
        value_cols(m).wait_recv()
        gv_pairs(m).wait_recv()
        both = cols_all[0, m].reshape(2 * share, 4 * tokens)
        for j in range(inner // (2 * TILE)):
            cols = slice(j * 2 * TILE, (j + 1) * 2 * TILE)
            acc[0, :, :, cols] += jnp.dot(
                both, rows_gv[m, :, cols], preferred_element_type=jnp.float32
            ).reshape(2, share, 2 * TILE)

    def grad_lanes(m, p):
        packed = cols_all[1, m, p]
        return [
            jnp.concatenate(
                [
                    packed[:, (2 * place_of + b) * half : (2 * place_of + b + 1) * half]
                    for place_of in range(4)
                ],
                axis=1,
            )
            for b in range(2)
        ]

    def out_product(m, p):
        @pl.when(p == 0)
        def _():
            v_pairs(m).wait_recv()

        grad_cols(m, p).wait_recv()
        both = jnp.concatenate(grad_lanes(m, p), axis=0)
        for j in range(inner // (2 * TILE)):
            cols = slice(j * 2 * TILE, (j + 1) * 2 * TILE)
            acc[1, :, :, cols] += jnp.dot(
                both, rows_v[m, p, :, cols], preferred_element_type=jnp.float32
            ).reshape(2, share, 2 * TILE)

    def transpose_weights():
        def tile(j, carry):
            wvt_ref[:, tile_at(j)] = wv_ref[tile_at(j)].T
            return carry

        lax.fori_loop(0, wide, tile, 0)

    @pl.when(top)
    def _():
        whole(0, 1, True)
        lax.fori_loop(1, micro, scales, 0)
        load_rest.wait()
        whole(1, 1, False)
        turn(0, 0)

        def pair(unit, carry):
            whole(unit * (CHUNKS // 2), CHUNKS // 2, False)
            turn(unit // 2, unit % 2)

            @pl.when(unit <= micro)
            def _():
                values(unit - 1)

            return carry

        lax.fori_loop(1, 2 * micro, pair, 0)

    def stage(t, carry):
        k = t - micro

        @pl.when(k >= 0)
        def _():
            @pl.when(k == 0)
            def _():
                load_wo.wait()
                transpose_weights()

            @pl.when(jnp.logical_and(section == 0, k == 0))
            def _():
                acc[...] = jnp.zeros_like(acc)
                relay_values()

            chain(k)

            @pl.when(jnp.logical_and(section == 0, k > 1))
            def _():
                relay_grads(k - 2)

            @pl.when(
                jnp.logical_and(
                    section == 0, jnp.logical_and(k > CHUNKS, k % CHUNKS == 2)
                )
            )
            def _():
                value_product(k // CHUNKS - 1)

            @pl.when(
                jnp.logical_and(
                    section == 0, jnp.logical_and(k >= CHUNKS, k % CHUNKS == 0)
                )
            )
            def _():
                gain_terms(k // CHUNKS - 1)

            @pl.when(
                jnp.logical_and(
                    section == 0,
                    jnp.logical_and(k > CHUNKS // 2, k % (CHUNKS // 2) == CHUNKS // 2 - 1),
                )
            )
            def _():
                unit = k // (CHUNKS // 2) - 1
                out_product(unit // 2, unit % 2)

        @pl.when(k < 0)
        def _():
            values(t)

        return carry

    @pl.when(section < sections - 1)
    def _():
        lax.fori_loop(0, steps + micro, stage, 0)

    @pl.when(section == 0)
    def _():
        relay_grads(steps - 2)
        gain_terms(micro - 1)

    gain_all[me] = jnp.sum(gain_part[...], axis=0, keepdims=True)
    for bits in range(1, peers):
        gain_copy(bits).start()

    @pl.when(section > 0)
    def _():
        acc[...] = jnp.zeros_like(acc)
        relay_values()

        def early(k, carry):
            relay_grads(k)
            return carry

        lax.fori_loop(0, steps - 1, early, 0)

        def heavy(m, carry):
            value_product(m)
            return carry

        lax.fori_loop(0, micro - 1, heavy, 0)

        def light(unit, carry):
            out_product(unit // 2, unit % 2)
            return carry

        lax.fori_loop(0, 2 * micro - 1, light, 0)

    relay_grads(steps - 1)
    last = micro - 1
    mine = coordinate(me, far[1])
    grad_cols(last, 1).wait_recv()
    lanes = grad_lanes(last, 1)
    give = jnp.where(mine == 0, lanes[1], lanes[0])
    keep = jnp.where(mine == 0, lanes[0], lanes[1])
    side = coordinate(me, far[0])
    for j in range(narrow):
        cols = slice(j * TILE, (j + 1) * TILE)
        part_out[1, j] = (
            acc[1, 1 - mine, :, cols]
            + jnp.dot(give, rows_v[last, 1, :, cols], preferred_element_type=jnp.float32)
        ).astype(jnp.bfloat16)
        part_copy(1, j).start()
        if j == 0:
            value_cols(last).wait_recv()
            gv_pairs(last).wait_recv()
        part_out[0, j] = (
            acc[0, 1 - side, :, cols]
            + jnp.dot(
                cols_all[0, last, 1 - side],
                rows_gv[last, :, cols],
                preferred_element_type=jnp.float32,
            )
        ).astype(jnp.bfloat16)
        part_copy(0, j).start()

    for j in range(narrow):
        cols = slice(j * TILE, (j + 1) * TILE)
        acc[1, mine, :, cols] += jnp.dot(
            keep, rows_v[last, 1, :, cols], preferred_element_type=jnp.float32
        )
        acc[0, side, :, cols] += jnp.dot(
            cols_all[0, last, side], rows_gv[last, :, cols], preferred_element_type=jnp.float32
        )

    gains().wait_recv()
    gained = gain_all[0]
    for owner in range(1, peers):
        gained = gained + gain_all[owner]
    gg_ref[...] = gained
    gv_all().wait_send()
    v_all().wait_send()
    for kind in (0, 1):
        cols_sent(kind).wait_send()

    @pl.when(section > 0)
    def _():
        remote(
            pass_buf, grad_buf, down_send.at[0], down_recv.at[0, 0], {"section": section - 1}
        ).wait_send()

    gains().wait_send()
    for j in range(narrow):
        cols = slice(j * TILE, (j + 1) * TILE)
        for kind, row, out_ref in ((1, mine, og_ref), (0, side, vg_ref)):
            part_copy(kind, j).wait_recv()
            out_ref[:, cols] = acc[kind, row, :, cols] + part_in[kind, j].astype(jnp.float32)

    for kind in (0, 1):
        remote(
            part_out.at[kind], part_in.at[kind], part_send.at[kind], part_recv.at[kind, 0], peer(1)
        ).wait_send()


def place_outputs(vg_ref, og_ref, gg_ref, vg_out, og_out, gg_out, sem):
    pairs = ((vg_ref, vg_out), (og_ref, og_out), (gg_ref, gg_out))
    copies = [
        pltpu.make_async_copy(source, target, sem.at[i])
        for i, (source, target) in enumerate(pairs)
    ]
    for copy in copies:
        copy.start()
    for copy in copies:
        copy.wait()


def fused(mesh, saved, cotangent, slot_table, gain, value_weight, out_weight):
    peers, sections = mesh.shape["seq"], mesh.shape["section"]
    micro, tokens, width = cotangent.shape
    inner = value_weight.shape[2]
    share = width // peers
    narrow = inner // TILE
    chunk = tokens // CHUNKS
    steps = micro * CHUNKS
    held = pl.BlockSpec(memory_space=pltpu.VMEM)
    far_off = pl.BlockSpec(memory_space=pl.ANY)
    value_grad, out_grad, gain_grad = pl.pallas_call(
        functools.partial(fused_kernel, peers, sections),
        out_shape=(
            jax.ShapeDtypeStruct((share, inner), jnp.float32),
            jax.ShapeDtypeStruct((share, inner), jnp.float32),
            jax.ShapeDtypeStruct((1, width), jnp.float32),
        ),
        in_specs=[
            far_off,
            far_off,
            far_off,
            held,
            far_off,
            far_off,
        ],
        out_specs=(held, held, held),
        scratch_shapes=[
            pltpu.VMEM((micro, tokens, width), jnp.bfloat16),
            pltpu.VMEM((width, inner), jnp.bfloat16),
            pltpu.VMEM((width, inner), jnp.bfloat16),
            pltpu.VMEM((inner, width), jnp.bfloat16),
            pltpu.VMEM((micro, tokens, 1), jnp.float32),
            pltpu.VMEM((micro, tokens, width), jnp.bfloat16),
            pltpu.VMEM((micro, tokens, width), jnp.bfloat16),
            pltpu.VMEM((tokens, width), jnp.bfloat16),
            pltpu.VMEM((tokens // 2, width), jnp.float32),
            pltpu.VMEM((micro, 4 * tokens, inner), jnp.bfloat16),
            pltpu.VMEM((micro, 2, 2 * tokens, inner), jnp.bfloat16),
            pltpu.VMEM((2, micro, width, tokens), jnp.bfloat16),
            pltpu.VMEM((2, micro, 2, share, 4 * tokens), jnp.bfloat16),
            pltpu.VMEM((2, 2, share, inner), jnp.float32),
            pltpu.VMEM((2, narrow, share, TILE), jnp.bfloat16),
            pltpu.VMEM((2, narrow, share, TILE), jnp.bfloat16),
            pltpu.VMEM((8, width), jnp.float32),
            pltpu.VMEM((peers, 1, width), jnp.float32),
            pltpu.SMEM((1, micro), jnp.int32),
            pltpu.SemaphoreType.DMA((5,)),
            pltpu.SemaphoreType.DMA((3,)),
            pltpu.SemaphoreType.DMA((1,)),
            pltpu.SemaphoreType.DMA((steps,)),
            pltpu.SemaphoreType.DMA((micro,)),
            pltpu.SemaphoreType.DMA((1,)),
            pltpu.SemaphoreType.DMA((micro,)),
            pltpu.SemaphoreType.DMA((micro,)),
            pltpu.SemaphoreType.DMA((2,)),
            pltpu.SemaphoreType.DMA((2, micro, 2)),
            pltpu.SemaphoreType.DMA((1,)),
            pltpu.SemaphoreType.DMA((steps, 3)),
            pltpu.SemaphoreType.DMA((2,)),
            pltpu.SemaphoreType.DMA((2, narrow)),
            pltpu.SemaphoreType.DMA((1,)),
            pltpu.SemaphoreType.DMA((1,)),
        ],
        compiler_params=pltpu.CompilerParams(
            collective_id=0, has_side_effects=True, vmem_limit_bytes=VMEM_BYTES
        ),
    )(slot_table, saved[0], cotangent, gain, value_weight[0], out_weight[0])
    value_grad, out_grad, gain_grad = pl.pallas_call(
        place_outputs,
        out_shape=(
            jax.ShapeDtypeStruct((share, inner), jnp.float32),
            jax.ShapeDtypeStruct((share, inner), jnp.float32),
            jax.ShapeDtypeStruct((1, width), jnp.float32),
        ),
        in_specs=[far_off] * 3,
        out_specs=(far_off,) * 3,
        scratch_shapes=[pltpu.SemaphoreType.DMA((3,))],
        compiler_params=pltpu.CompilerParams(vmem_limit_bytes=8 * 1024 * 1024),
    )(value_grad, out_grad, gain_grad)
    return value_grad[None], out_grad[None], gain_grad


def fits(mesh, saved, cotangent, slot_table, gain, value_weight, out_weight):
    peers = mesh.shape["seq"]
    micro, tokens, width = cotangent.shape
    inner = value_weight.shape[2]
    share = width // peers
    held = 6 * width * inner + 2 * 2 * micro * 4 * tokens * (inner + 2 * share)
    held += 2 * micro * tokens * width * 5 + 6 * tokens * width
    held += share * inner * (4 * 4 + 4 * 2 + 4 * 2)
    return (
        peers == 8
        and micro > 1
        and tokens == LANES
        and width % (3 * TILE) == 0
        and width >= 6 * TILE
        and inner % (2 * TILE) == 0
        and width % (16 * peers) == 0
        and held < VMEM_BYTES - 2 * 1024 * 1024
    )


def on_device(mesh, *arrays):
    if fits(mesh, *arrays):
        return fused(mesh, *arrays)
    return per_device(*arrays)


def solution(mesh):
    in_specs = (
        P("section", None, "seq", None),
        P(None, "seq", None),
        P("section", None),
        P("section", None),
        P("section", None, None),
        P("section", None, None),
    )
    out_specs = (P("section", "seq", None), P("section", "seq", None), P("section", None))
    return jax.shard_map(
        functools.partial(on_device, mesh), mesh=mesh, in_specs=in_specs, out_specs=out_specs, check_vma=False
    )
```

```python
import functools

import jax
import jax.numpy as jnp
from jax import lax
from jax.experimental import pallas as pl
from jax.experimental.pallas import tpu as pltpu
from jax.sharding import PartitionSpec as P

EPSILON = 1e-06


def passed_along(value, axis, steps):
    count = lax.axis_size(axis)
    first, last = (max(0, -steps), min(count, count - steps))
    return lax.ppermute(value, axis, [(source, source + steps) for source in range(first, last)])


def normalize(inputs, gain_row):
    value_rows = inputs.astype(jnp.float32)
    inv_rms = lax.rsqrt(jnp.mean(value_rows * value_rows, axis=-1, keepdims=True) + EPSILON)
    unit_rows = value_rows * inv_rms
    return (unit_rows, inv_rms, (unit_rows * gain_row).astype(jnp.bfloat16))


def input_grads(inputs, grad_out, gain_row, w_value, w_out):
    unit_rows, inv_rms, normed = normalize(inputs, gain_row)
    grad_value = jnp.dot(grad_out, w_out, preferred_element_type=jnp.float32).astype(jnp.bfloat16)
    grad_normed = lax.dot_general(
        grad_value, w_value, (((1,), (1,)), ((), ())), preferred_element_type=jnp.float32
    )
    gain_term = jnp.sum(grad_normed * unit_rows, axis=0)
    grad_unit = grad_normed * gain_row
    grad_in = grad_out.astype(jnp.float32) + inv_rms * (
        grad_unit - unit_rows * jnp.mean(grad_unit * unit_rows, axis=-1, keepdims=True)
    )
    return (grad_in.astype(jnp.bfloat16), grad_value, normed, gain_term)


def arrivals(
    step_index, sent, section_count, section_index, micro_count, cotangent, local_saved, slot_order
):
    if step_index > 0:
        incoming = passed_along(sent, "section", -1)
    else:
        incoming = sent
    micro_index = step_index - (section_count - 1 - section_index)
    active_now = jnp.logical_and(micro_index >= 0, micro_index < micro_count)
    clipped = jnp.clip(micro_index, 0, micro_count - 1)
    top_grad = lax.dynamic_index_in_dim(cotangent, clipped, 0, keepdims=False)
    grad_out = jnp.where(section_index == section_count - 1, top_grad, incoming)
    slot_index = lax.dynamic_index_in_dim(slot_order, clipped, 0, keepdims=False)
    inputs = lax.dynamic_index_in_dim(local_saved, slot_index, 0, keepdims=False)
    return (active_now, clipped, grad_out, inputs)


def per_device(saved, cotangent, slot_table, gain, value_weight, out_weight):
    section_count = lax.axis_size("section")
    section_index = lax.axis_index("section")
    micro_count = slot_table.shape[1]
    local_saved = saved[0]
    slot_order = slot_table[0]
    gain_row = gain[0]
    w_value = value_weight[0]
    w_out = out_weight[0]
    token_rows = cotangent.shape[1]
    model_width = w_value.shape[0]
    inner_width = w_value.shape[1]
    sent = jnp.zeros((token_rows, model_width), jnp.bfloat16)
    gain_acc = jnp.zeros((model_width,), jnp.float32)
    out_stash = jnp.zeros((micro_count, token_rows, model_width), jnp.bfloat16)
    value_stash = jnp.zeros((micro_count, token_rows, inner_width), jnp.bfloat16)
    for step_index in range(micro_count + section_count - 1):
        active_now, clipped, grad_out, inputs = arrivals(
            step_index,
            sent,
            section_count,
            section_index,
            micro_count,
            cotangent,
            local_saved,
            slot_order,
        )

        def working(carried):
            grad_in, grad_value, normed, gain_term = input_grads(
                inputs, grad_out, gain_row, w_value, w_out
            )
            new_out = lax.dynamic_update_index_in_dim(carried[2], grad_out, clipped, 0)
            new_value = lax.dynamic_update_index_in_dim(carried[3], grad_value, clipped, 0)
            return (grad_in, carried[1] + gain_term, new_out, new_value)

        def resting(carried):
            return carried

        sent, gain_acc, out_stash, value_stash = lax.cond(
            active_now, working, resting, (sent, gain_acc, out_stash, value_stash)
        )
    ordered = jnp.take(local_saved, slot_order, axis=0).reshape(
        micro_count * token_rows, model_width
    )
    unit_all, inv_all, normed_all = normalize(ordered, gain_row)
    values_all = jnp.dot(normed_all, w_value, preferred_element_type=jnp.float32).astype(
        jnp.bfloat16
    )
    grads_all = out_stash.reshape(micro_count * token_rows, model_width)
    grad_values = value_stash.reshape(micro_count * token_rows, inner_width)
    value_acc = lax.dot_general(
        normed_all, grad_values, (((0,), (0,)), ((), ())), preferred_element_type=jnp.float32
    )
    out_acc = lax.dot_general(
        grads_all, values_all, (((0,), (0,)), ((), ())), preferred_element_type=jnp.float32
    )
    value_grad, out_grad = (
        lax.psum_scatter(value_acc, "seq", scatter_dimension=0, tiled=True),
        lax.psum_scatter(out_acc, "seq", scatter_dimension=0, tiled=True),
    )
    gain_total = lax.psum(gain_acc, "seq")
    return (value_grad[None], out_grad[None], gain_total[None])


TILE = 256
LANES = 128
CHUNKS = 4
VMEM_BYTES = 50 * 1024 * 1024


def flipped(index, bits, count):
    total, unit = 0, 1
    while unit < count:
        total = total + ((index // unit + (bits // unit) % 2) % 2) * unit
        unit *= 2
    return total


def tile_at(index, size=TILE):
    return pl.ds(pl.multiple_of(index * size, size), size)


def fused_kernel(
    peers,
    sections,
    slot_hbm,
    saved_hbm,
    cot_hbm,
    gain_ref,
    wv_hbm,
    wo_hbm,
    vg_ref,
    og_ref,
    gg_ref,
    saved_ref,
    wv_ref,
    wo_ref,
    wvt_ref,
    inv_buf,
    grad_buf,
    pass_buf,
    normed,
    gn,
    rows_gv,
    rows_v,
    turned,
    cols_all,
    acc,
    part_out,
    part_in,
    gain_part,
    gain_all,
    slot_ref,
    load_sem,
    wv_sem,
    gv_send,
    gv_chip,
    gv_pair,
    v_send,
    v_chip,
    v_pair,
    cols_send,
    cols_recv,
    down_send,
    down_recv,
    part_send,
    part_recv,
    gain_send,
    gain_recv,
):
    section = lax.axis_index("section")
    me = lax.axis_index("seq")
    micro, tokens, width = grad_buf.shape
    inner = wv_ref.shape[1]
    share = width // peers
    wide, narrow = width // TILE, inner // TILE
    third = width // 3
    edges = [TILE * at for at in (0, wide // 3, wide - wide // 3, wide)]
    groups = [slice(low, high) for low, high in zip(edges[:-1], edges[1:])]
    chunk, half = tokens // CHUNKS, tokens // 2
    steps = micro * CHUNKS
    top = section == sections - 1
    near = (peers // 4, peers // 2)
    far = (peers // 2, peers // 4)

    def peer(bits):
        return {"seq": flipped(me, bits, peers)}

    def coordinate(device, bit):
        return (device // bit) % 2

    def place(kind, device):
        return coordinate(device, near[kind]) * 2 + device % 2

    def remote(source, target, send_sem, recv_sem, device):
        return pltpu.make_async_remote_copy(
            src_ref=source,
            dst_ref=target,
            send_sem=send_sem,
            recv_sem=recv_sem,
            device_id=device,
            device_id_type=pl.DeviceIdType.MESH,
        )

    def gv_copy(k, owner, recv_sem, bits):
        m, h = k // CHUNKS, k % CHUNKS
        spot = rows_gv.at[m, tile_at(place(0, owner) * CHUNKS + h, chunk)]
        return remote(spot, spot, gv_send.at[0], recv_sem, peer(bits))

    def gv_to_chip(k):
        return gv_copy(k, me, gv_chip.at[k], near[0])

    def gv_from_chip(k):
        return gv_copy(k, flipped(me, near[0], peers), gv_chip.at[k], near[0])

    def gv_to_core(k):
        return gv_copy(k, me, gv_pair.at[k // CHUNKS], 1)

    def gv_relay(k):
        return gv_copy(k, flipped(me, near[0], peers), gv_pair.at[k // CHUNKS], 1)

    def gv_pairs(m):
        spot = rows_gv.at[m, : 2 * tokens]
        return remote(spot, spot, gv_send.at[0], gv_pair.at[m], peer(1))

    def gv_all():
        spot = rows_gv.at[:, : 3 * tokens]
        return remote(spot, spot, gv_send.at[0], gv_pair.at[0], peer(1))

    def v_copy(m, owner, recv_sem, bits):
        spot = rows_v.at[m, :, tile_at(place(1, owner), half)]
        return remote(spot, spot, v_send.at[0], recv_sem, peer(bits))

    def v_to_chip(m):
        return v_copy(m, me, v_chip.at[m], near[1])

    def v_from_chip(m):
        return v_copy(m, flipped(me, near[1], peers), v_chip.at[m], near[1])

    def v_to_core(m):
        return v_copy(m, me, v_pair.at[m], 1)

    def v_relay(m):
        return v_copy(m, flipped(me, near[1], peers), v_pair.at[m], 1)

    def v_pairs(m):
        spot = rows_v.at[m, :, : 2 * half]
        return remote(spot, spot, v_send.at[0], v_pair.at[m], peer(1))

    def v_all():
        spot = rows_v.at[:, :, : 3 * half]
        return remote(spot, spot, v_send.at[0], v_pair.at[0], peer(1))

    def ways(kind):
        return (near[kind], near[kind] + 1, 1)

    def col_source(kind, m, part, target):
        if kind == 0:
            block = target + (part - coordinate(target, far[0])) * far[0]
        else:
            block = part * 4 + place(1, target)
        return turned.at[kind, m, tile_at(block, share)]

    def col_copy(kind, m, part, bits):
        return remote(
            col_source(kind, m, part, flipped(me, bits, peers)),
            cols_all.at[kind, m, part, :, tile_at(place(kind, me), tokens)],
            cols_send.at[kind],
            cols_recv.at[kind, m, part if kind == 1 else 0],
            peer(bits),
        )

    def send_cols(kind, m, parts):
        for bits in ways(kind):
            for part in parts:
                col_copy(kind, m, part, bits).start()
        for part in parts:
            cols_all[kind, m, part, :, tile_at(place(kind, me), tokens)] = col_source(
                kind, m, part, me
            )[...]

    def value_cols(m):
        spot = cols_all.at[0, m, :, :, : 3 * tokens]
        return remote(spot, spot, cols_send.at[0], cols_recv.at[0, m, 0], peer(1))

    def grad_cols(m, p):
        spot = cols_all.at[1, m, p, :, : 3 * tokens]
        return remote(spot, spot, cols_send.at[1], cols_recv.at[1, m, p], peer(1))

    def cols_sent(kind):
        spot = cols_all.at[kind, :, :, :, : 3 * tokens]
        return remote(spot, spot, cols_send.at[kind], cols_recv.at[kind, 0, 0], peer(1))

    def down_copy(k, g, target):
        spot, cols = tile_at(k % CHUNKS, chunk), groups[g]
        return remote(
            pass_buf.at[k // CHUNKS, spot, cols],
            grad_buf.at[k // CHUNKS, spot, cols],
            down_send.at[0],
            down_recv.at[k, g],
            {"section": target},
        )

    def part_copy(kind, j):
        return remote(
            part_out.at[kind, j],
            part_in.at[kind, j],
            part_send.at[kind],
            part_recv.at[kind, j],
            peer(far[kind]),
        )

    def gain_copy(bits):
        spot = gain_all.at[me]
        return remote(spot, spot, gain_send.at[0], gain_recv.at[0], peer(bits))

    def gains():
        spot = gain_all.at[: peers - 1]
        return remote(spot, spot, gain_send.at[0], gain_recv.at[0], peer(1))

    load_saved = pltpu.make_async_copy(saved_hbm, saved_ref, load_sem.at[0])
    load_slot = pltpu.make_async_copy(slot_hbm, slot_ref, load_sem.at[4])
    load_wo = pltpu.make_async_copy(wo_hbm, wo_ref, load_sem.at[1])
    load_first = pltpu.make_async_copy(cot_hbm.at[0], grad_buf.at[0], load_sem.at[2])
    load_rest = pltpu.make_async_copy(cot_hbm.at[1:], grad_buf.at[1:], load_sem.at[3])

    def load_wv(j):
        rows = slice(j * third, (j + 1) * third)
        return pltpu.make_async_copy(wv_hbm.at[rows], wv_ref.at[rows], wv_sem.at[j])

    @pl.when(top)
    def _():
        load_first.start()
        load_wo.start()

    @pl.when(section < sections - 1)
    def _():
        load_saved.start()
        for j in range(3):
            load_wv(j).start()
        load_wo.start()

    load_slot.start()
    barrier = pltpu.get_barrier_semaphore()
    for bits in range(1, peers):
        pl.semaphore_signal(
            barrier, inc=1, device_id=peer(bits), device_id_type=pl.DeviceIdType.MESH
        )

    @pl.when(section > 0)
    def _():
        pl.semaphore_signal(
            barrier,
            inc=1,
            device_id={"section": section - 1},
            device_id_type=pl.DeviceIdType.MESH,
        )

    @pl.when(section < sections - 1)
    def _():
        pl.semaphore_signal(
            barrier,
            inc=1,
            device_id={"section": section + 1},
            device_id_type=pl.DeviceIdType.MESH,
        )

    gain_part[...] = jnp.zeros_like(gain_part)

    @pl.when(top)
    def _():
        load_first.wait()
        load_saved.start()
        load_wv(0).start()

    @pl.when(section < sections - 1)
    def _():
        load_saved.wait()

    load_slot.wait()

    def scales(m, carry):
        slot = slot_ref[0, m]
        total = jnp.zeros((tokens, LANES), jnp.float32)
        for j in range(width // LANES):
            x = saved_ref[slot, :, j * LANES : (j + 1) * LANES].astype(jnp.float32)
            total = total + x * x
        total = jnp.sum(total, axis=1, keepdims=True)
        inv_buf[m] = lax.rsqrt(total / width + EPSILON)
        return carry

    @pl.when(section < sections - 1)
    def _():
        lax.fori_loop(0, micro, scales, 0)

    pl.semaphore_wait(
        barrier,
        peers - 1
        + (section > 0).astype(jnp.int32)
        + (section < sections - 1).astype(jnp.int32),
    )

    @pl.when(top)
    def _():
        load_wo.wait()
        load_wv(1).start()
        load_wv(2).start()
        load_rest.start()

    @pl.when(section < sections - 1)
    def _():
        for j in range(3):
            load_wv(j).wait()

    def values(m):
        slot = slot_ref[0, m]
        inv = inv_buf[m]
        for j in range(wide):
            cols = slice(j * TILE, (j + 1) * TILE)
            x = saved_ref[slot, :, cols].astype(jnp.float32)
            n = (x * inv * gain_ref[:, cols]).astype(jnp.bfloat16)
            normed[:, cols] = n
            turned[0, m, cols] = n.T
        result = jnp.dot(
            normed[...], wv_ref[...], preferred_element_type=jnp.float32
        ).astype(jnp.bfloat16)
        for p in range(2):
            rows_v[m, p, tile_at(place(1, me), half)] = result[p * half : (p + 1) * half]

    def share_values(m):
        send_cols(0, m, (0, 1))
        v_to_chip(m).start()
        v_to_core(m).start()

    def turn(m, p):
        block = width // 4
        for y in range(2):
            left, right = (
                grad_buf[m, tile_at(p, half), :].T[(2 * y + i) * block : (2 * y + i + 1) * block]
                for i in range(2)
            )
            turned[1, m, tile_at(p * 2 + y, block)] = jnp.concatenate([left, right], axis=1)

        @pl.when(p == 0)
        def _():
            send_cols(1, m, (0,))

        @pl.when(p == 1)
        def _():
            send_cols(1, m, (1,))

    def dispatch(k, count, grad_value):
        m, h = k // CHUNKS, k % CHUNKS
        spot = place(0, me) * CHUNKS + h
        for i in range(count):
            rows_gv[m, tile_at(spot + i, chunk)] = grad_value[i * chunk : (i + 1) * chunk].astype(
                jnp.bfloat16
            )
        for i in range(count):
            gv_to_chip(k + i).start()
            gv_to_core(k + i).start()

    def whole(k, count, first):
        m, h = k // CHUNKS, k % CHUNKS
        rows = count * chunk
        here = tile_at(h // count, rows)
        slot = slot_ref[0, m]
        dispatch(
            k,
            count,
            jnp.dot(grad_buf[m, here], wo_ref[...], preferred_element_type=jnp.float32),
        )
        if first:
            load_saved.wait()
            scales(0, 0)
        inv = inv_buf[m, here]
        grad_value = rows_gv[m, tile_at((place(0, me) * CHUNKS + h) // count, rows)]
        total = jnp.zeros((rows, LANES), jnp.float32)
        for j in range(3):
            cols = slice(j * third, (j + 1) * third)
            if first:
                load_wv(j).wait()
            term = lax.dot_general(
                grad_value,
                wv_ref[cols],
                (((1,), (1,)), ((), ())),
                preferred_element_type=jnp.float32,
            )
            unit = saved_ref[slot, here, cols].astype(jnp.float32) * inv
            grad_unit = term * gain_ref[:, cols]
            gn[:rows, cols] = grad_unit
            gain_part[:, cols] += jnp.sum((term * unit).reshape(rows // 8, 8, third), axis=0)
            both = grad_unit * unit
            for i in range(third // LANES):
                total = total + both[:, i * LANES : (i + 1) * LANES]
        pull = inv * inv * (jnp.sum(total, axis=1, keepdims=True) / width)
        for j in range(3):
            cols = slice(j * third, (j + 1) * third)
            pass_buf[m, here, cols] = (
                grad_buf[m, here, cols].astype(jnp.float32)
                + inv * gn[:rows, cols]
                - saved_ref[slot, here, cols].astype(jnp.float32) * pull
            ).astype(jnp.bfloat16)
        for i in range(count):
            for g in range(len(groups)):
                down_copy(k + i, g, section - 1).start()

    def chain(k):
        m, h = k // CHUNKS, k % CHUNKS
        here = tile_at(h, chunk)
        slot = slot_ref[0, m]
        inv = inv_buf[m, here]
        mine = tile_at(place(0, me) * CHUNKS + h, chunk)
        turning = (h % (CHUNKS // 2)) == CHUNKS // 2 - 1
        total = jnp.zeros((chunk, inner), jnp.float32)
        for g, cols in enumerate(groups):
            down_copy(k, g, section + 1).wait_recv()
            if g == len(groups) - 1:

                @pl.when(jnp.logical_and(section == 0, turning))
                def _():
                    turn(m, h // (CHUNKS // 2))

            total = total + jnp.dot(
                grad_buf[m, here, cols], wo_ref[cols], preferred_element_type=jnp.float32
            )
        dispatch(k, 1, total)

        @pl.when(section > 0)
        def _():
            grad_value = rows_gv[m, mine]
            own = place(1, me) * (CHUNKS // 2) + h % (CHUNKS // 2)
            value = rows_v[m, h // (CHUNKS // 2), tile_at(own, chunk)]
            dots = jnp.sum(
                grad_value.astype(jnp.float32) * value.astype(jnp.float32), axis=1, keepdims=True
            )
            pull = inv * inv * (dots / width)
            for g, cols in enumerate(groups):
                term = jnp.dot(grad_value, wvt_ref[:, cols], preferred_element_type=jnp.float32)
                x = saved_ref[slot, here, cols].astype(jnp.float32)
                pass_buf[m, here, cols] = (
                    grad_buf[m, here, cols].astype(jnp.float32)
                    + inv * (term * gain_ref[:, cols])
                    - x * pull
                ).astype(jnp.bfloat16)
                down_copy(k, g, section - 1).start()
                gain_part[:, cols] += jnp.sum(
                    (term * (x * inv)).reshape(chunk // 8, 8, cols.stop - cols.start), axis=0
                )

        @pl.when(jnp.logical_and(section > 0, turning))
        def _():
            turn(m, h // (CHUNKS // 2))

    def gain_terms(m):
        slot = slot_ref[0, m]
        inv = inv_buf[m]
        grad_value = rows_gv[m, tile_at(place(0, me), tokens)]
        for j in range(3):
            cols = slice(j * third, (j + 1) * third)
            term = jnp.dot(grad_value, wvt_ref[:, cols], preferred_element_type=jnp.float32)
            unit = saved_ref[slot, :, cols].astype(jnp.float32) * inv
            gain_part[:, cols] += jnp.sum((term * unit).reshape(tokens // 8, 8, third), axis=0)

    def relay_values():
        def one(m, carry):
            v_from_chip(m).wait_recv()
            v_relay(m).start()
            return carry

        lax.fori_loop(0, micro, one, 0)

    def relay_grads(k):
        gv_from_chip(k).wait_recv()
        gv_relay(k).start()

    def value_product(m):
        value_cols(m).wait_recv()
        gv_pairs(m).wait_recv()
        both = cols_all[0, m].reshape(2 * share, 4 * tokens)
        for j in range(inner // (2 * TILE)):
            cols = slice(j * 2 * TILE, (j + 1) * 2 * TILE)
            acc[0, :, :, cols] += jnp.dot(
                both, rows_gv[m, :, cols], preferred_element_type=jnp.float32
            ).reshape(2, share, 2 * TILE)

    def grad_lanes(m, p):
        packed = cols_all[1, m, p]
        return [
            jnp.concatenate(
                [
                    packed[:, (2 * place_of + b) * half : (2 * place_of + b + 1) * half]
                    for place_of in range(4)
                ],
                axis=1,
            )
            for b in range(2)
        ]

    def out_product(m, p):
        @pl.when(p == 0)
        def _():
            v_pairs(m).wait_recv()

        grad_cols(m, p).wait_recv()
        both = jnp.concatenate(grad_lanes(m, p), axis=0)
        for j in range(inner // (2 * TILE)):
            cols = slice(j * 2 * TILE, (j + 1) * 2 * TILE)
            acc[1, :, :, cols] += jnp.dot(
                both, rows_v[m, p, :, cols], preferred_element_type=jnp.float32
            ).reshape(2, share, 2 * TILE)

    def transpose_weights():
        def tile(j, carry):
            wvt_ref[:, tile_at(j)] = wv_ref[tile_at(j)].T
            return carry

        lax.fori_loop(0, wide, tile, 0)

    @pl.when(top)
    def _():
        whole(0, 1, True)
        lax.fori_loop(1, micro, scales, 0)
        load_rest.wait()
        whole(1, 1, False)
        turn(0, 0)

        def pair(unit, carry):
            whole(unit * (CHUNKS // 2), CHUNKS // 2, False)
            turn(unit // 2, unit % 2)

            @pl.when(unit <= micro)
            def _():
                values(unit - 1)
                share_values(unit - 1)

            return carry

        lax.fori_loop(1, 2 * micro, pair, 0)

    def stage(t, carry):
        k = t - micro

        @pl.when(k >= 0)
        def _():
            @pl.when(k == 0)
            def _():
                load_wo.wait()
                transpose_weights()

            @pl.when(jnp.logical_and(section == 0, k == 0))
            def _():
                acc[...] = jnp.zeros_like(acc)
                relay_values()

            chain(k)

            @pl.when(
                jnp.logical_and(
                    section > 0, jnp.logical_and(k % CHUNKS == 1, k < CHUNKS * (micro - 1))
                )
            )
            def _():
                share_values(k // CHUNKS + 1)

            @pl.when(jnp.logical_and(section == 0, k > 1))
            def _():
                relay_grads(k - 2)

            @pl.when(
                jnp.logical_and(
                    section == 0, jnp.logical_and(k > CHUNKS, k % CHUNKS == 2)
                )
            )
            def _():
                value_product(k // CHUNKS - 1)

            @pl.when(
                jnp.logical_and(
                    section == 0, jnp.logical_and(k >= CHUNKS, k % CHUNKS == 0)
                )
            )
            def _():
                gain_terms(k // CHUNKS - 1)

            @pl.when(
                jnp.logical_and(
                    section == 0,
                    jnp.logical_and(k > CHUNKS // 2, k % (CHUNKS // 2) == CHUNKS // 2 - 1),
                )
            )
            def _():
                unit = k // (CHUNKS // 2) - 1
                out_product(unit // 2, unit % 2)

        @pl.when(k < 0)
        def _():
            values(t)

            @pl.when(jnp.logical_or(section == 0, t == 0))
            def _():
                share_values(t)

        return carry

    @pl.when(section < sections - 1)
    def _():
        lax.fori_loop(0, steps + micro, stage, 0)

    @pl.when(section == 0)
    def _():
        relay_grads(steps - 2)
        gain_terms(micro - 1)

    gain_all[me] = jnp.sum(gain_part[...], axis=0, keepdims=True)
    for bits in range(1, peers):
        gain_copy(bits).start()

    @pl.when(section > 0)
    def _():
        acc[...] = jnp.zeros_like(acc)
        relay_values()

        def early(k, carry):
            relay_grads(k)
            return carry

        lax.fori_loop(0, steps - 1, early, 0)

        def heavy(m, carry):
            value_product(m)
            return carry

        lax.fori_loop(0, micro - 1, heavy, 0)

        def light(unit, carry):
            out_product(unit // 2, unit % 2)
            return carry

        lax.fori_loop(0, 2 * micro - 1, light, 0)

    relay_grads(steps - 1)
    last = micro - 1
    mine = coordinate(me, far[1])
    grad_cols(last, 1).wait_recv()
    lanes = grad_lanes(last, 1)
    give = jnp.where(mine == 0, lanes[1], lanes[0])
    keep = jnp.where(mine == 0, lanes[0], lanes[1])
    side = coordinate(me, far[0])
    for j in range(narrow):
        cols = slice(j * TILE, (j + 1) * TILE)
        part_out[1, j] = (
            acc[1, 1 - mine, :, cols]
            + jnp.dot(give, rows_v[last, 1, :, cols], preferred_element_type=jnp.float32)
        ).astype(jnp.bfloat16)
        part_copy(1, j).start()
        if j == 0:
            value_cols(last).wait_recv()
            gv_pairs(last).wait_recv()
        part_out[0, j] = (
            acc[0, 1 - side, :, cols]
            + jnp.dot(
                cols_all[0, last, 1 - side],
                rows_gv[last, :, cols],
                preferred_element_type=jnp.float32,
            )
        ).astype(jnp.bfloat16)
        part_copy(0, j).start()

    for j in range(narrow):
        cols = slice(j * TILE, (j + 1) * TILE)
        acc[1, mine, :, cols] += jnp.dot(
            keep, rows_v[last, 1, :, cols], preferred_element_type=jnp.float32
        )
        acc[0, side, :, cols] += jnp.dot(
            cols_all[0, last, side], rows_gv[last, :, cols], preferred_element_type=jnp.float32
        )

    gains().wait_recv()
    gained = gain_all[0]
    for owner in range(1, peers):
        gained = gained + gain_all[owner]
    gg_ref[...] = gained
    gv_all().wait_send()
    v_all().wait_send()
    for kind in (0, 1):
        cols_sent(kind).wait_send()

    @pl.when(section > 0)
    def _():
        remote(
            pass_buf, grad_buf, down_send.at[0], down_recv.at[0, 0], {"section": section - 1}
        ).wait_send()

    gains().wait_send()
    for j in range(narrow):
        cols = slice(j * TILE, (j + 1) * TILE)
        for kind, row, out_ref in ((1, mine, og_ref), (0, side, vg_ref)):
            part_copy(kind, j).wait_recv()
            out_ref[:, cols] = acc[kind, row, :, cols] + part_in[kind, j].astype(jnp.float32)

    for kind in (0, 1):
        remote(
            part_out.at[kind], part_in.at[kind], part_send.at[kind], part_recv.at[kind, 0], peer(1)
        ).wait_send()


def place_outputs(vg_ref, og_ref, gg_ref, vg_out, og_out, gg_out, sem):
    pairs = ((vg_ref, vg_out), (og_ref, og_out), (gg_ref, gg_out))
    copies = [
        pltpu.make_async_copy(source, target, sem.at[i])
        for i, (source, target) in enumerate(pairs)
    ]
    for copy in copies:
        copy.start()
    for copy in copies:
        copy.wait()


def fused(mesh, saved, cotangent, slot_table, gain, value_weight, out_weight):
    peers, sections = mesh.shape["seq"], mesh.shape["section"]
    micro, tokens, width = cotangent.shape
    inner = value_weight.shape[2]
    share = width // peers
    narrow = inner // TILE
    chunk = tokens // CHUNKS
    steps = micro * CHUNKS
    held = pl.BlockSpec(memory_space=pltpu.VMEM)
    far_off = pl.BlockSpec(memory_space=pl.ANY)
    value_grad, out_grad, gain_grad = pl.pallas_call(
        functools.partial(fused_kernel, peers, sections),
        out_shape=(
            jax.ShapeDtypeStruct((share, inner), jnp.float32),
            jax.ShapeDtypeStruct((share, inner), jnp.float32),
            jax.ShapeDtypeStruct((1, width), jnp.float32),
        ),
        in_specs=[
            far_off,
            far_off,
            far_off,
            held,
            far_off,
            far_off,
        ],
        out_specs=(held, held, held),
        scratch_shapes=[
            pltpu.VMEM((micro, tokens, width), jnp.bfloat16),
            pltpu.VMEM((width, inner), jnp.bfloat16),
            pltpu.VMEM((width, inner), jnp.bfloat16),
            pltpu.VMEM((inner, width), jnp.bfloat16),
            pltpu.VMEM((micro, tokens, 1), jnp.float32),
            pltpu.VMEM((micro, tokens, width), jnp.bfloat16),
            pltpu.VMEM((micro, tokens, width), jnp.bfloat16),
            pltpu.VMEM((tokens, width), jnp.bfloat16),
            pltpu.VMEM((tokens // 2, width), jnp.float32),
            pltpu.VMEM((micro, 4 * tokens, inner), jnp.bfloat16),
            pltpu.VMEM((micro, 2, 2 * tokens, inner), jnp.bfloat16),
            pltpu.VMEM((2, micro, width, tokens), jnp.bfloat16),
            pltpu.VMEM((2, micro, 2, share, 4 * tokens), jnp.bfloat16),
            pltpu.VMEM((2, 2, share, inner), jnp.float32),
            pltpu.VMEM((2, narrow, share, TILE), jnp.bfloat16),
            pltpu.VMEM((2, narrow, share, TILE), jnp.bfloat16),
            pltpu.VMEM((8, width), jnp.float32),
            pltpu.VMEM((peers, 1, width), jnp.float32),
            pltpu.SMEM((1, micro), jnp.int32),
            pltpu.SemaphoreType.DMA((5,)),
            pltpu.SemaphoreType.DMA((3,)),
            pltpu.SemaphoreType.DMA((1,)),
            pltpu.SemaphoreType.DMA((steps,)),
            pltpu.SemaphoreType.DMA((micro,)),
            pltpu.SemaphoreType.DMA((1,)),
            pltpu.SemaphoreType.DMA((micro,)),
            pltpu.SemaphoreType.DMA((micro,)),
            pltpu.SemaphoreType.DMA((2,)),
            pltpu.SemaphoreType.DMA((2, micro, 2)),
            pltpu.SemaphoreType.DMA((1,)),
            pltpu.SemaphoreType.DMA((steps, 3)),
            pltpu.SemaphoreType.DMA((2,)),
            pltpu.SemaphoreType.DMA((2, narrow)),
            pltpu.SemaphoreType.DMA((1,)),
            pltpu.SemaphoreType.DMA((1,)),
        ],
        compiler_params=pltpu.CompilerParams(
            collective_id=0, has_side_effects=True, vmem_limit_bytes=VMEM_BYTES
        ),
    )(slot_table, saved[0], cotangent, gain, value_weight[0], out_weight[0])
    value_grad, out_grad, gain_grad = pl.pallas_call(
        place_outputs,
        out_shape=(
            jax.ShapeDtypeStruct((share, inner), jnp.float32),
            jax.ShapeDtypeStruct((share, inner), jnp.float32),
            jax.ShapeDtypeStruct((1, width), jnp.float32),
        ),
        in_specs=[far_off] * 3,
        out_specs=(far_off,) * 3,
        scratch_shapes=[pltpu.SemaphoreType.DMA((3,))],
        compiler_params=pltpu.CompilerParams(vmem_limit_bytes=8 * 1024 * 1024),
    )(value_grad, out_grad, gain_grad)
    return value_grad[None], out_grad[None], gain_grad


def fits(mesh, saved, cotangent, slot_table, gain, value_weight, out_weight):
    peers = mesh.shape["seq"]
    micro, tokens, width = cotangent.shape
    inner = value_weight.shape[2]
    share = width // peers
    held = 6 * width * inner + 2 * 2 * micro * 4 * tokens * (inner + 2 * share)
    held += 2 * micro * tokens * width * 5 + 6 * tokens * width
    held += share * inner * (4 * 4 + 4 * 2 + 4 * 2)
    return (
        peers == 8
        and micro > 1
        and tokens == LANES
        and width % (3 * TILE) == 0
        and width >= 6 * TILE
        and inner % (2 * TILE) == 0
        and width % (16 * peers) == 0
        and held < VMEM_BYTES - 2 * 1024 * 1024
    )


def on_device(mesh, *arrays):
    if fits(mesh, *arrays):
        return fused(mesh, *arrays)
    return per_device(*arrays)


def solution(mesh):
    in_specs = (
        P("section", None, "seq", None),
        P(None, "seq", None),
        P("section", None),
        P("section", None),
        P("section", None, None),
        P("section", None, None),
    )
    out_specs = (P("section", "seq", None), P("section", "seq", None), P("section", None))
    return jax.shard_map(
        functools.partial(on_device, mesh), mesh=mesh, in_specs=in_specs, out_specs=out_specs, check_vma=False
    )
```
